32 devices in a mesh: gx: 2 (over y), gy: 16 (over z, x, core).
Axes of the slice: x: 2, y: 2, z: 4, core: 2. Of those that a mesh axis runs over, the one named last changes fastest.
Arguments:
- density: float32 [2, 512, 4096], P(None, 'gx', 'gy'), may hold values from -6 to 6
- observed: float32 [512, 4096], P('gx', 'gy'), may hold values from -6 to 6
- stations: int32 [512, 4096], P('gx', 'gy'), may hold values 0 or 1
- layer_index: int32 [2], replicated, may hold values from 0 to 511
Outputs:
- predicted: float32 [512, 4096], P('gx', 'gy')
- residual: float32 [512, 4096], P('gx', 'gy')
- gradient: float32 [2, 512, 4096], P(None, 'gx', 'gy')
The draws below stay inside these ranges and needn't reach their ends.
All inputs are finite; a program needn't handle non-finite values. No bound on the sum of `stations` on one device may be relied on, other than what follows from the above.
Results may differ from the reference program's by a relative error of at most 0.00016.
Values sent between devices are 32-bit elements; how exact they have to be, the bound alone decides.
No kernel may reach another device: no remote copies, remote signals or barrier semaphores. Data moves between devices by JAX's collectives and lax.ppermute only.
A program may use at most 64 MiB of HBM per device.

```python
import jax
import jax.numpy as jnp

LAYERS = 2
RADIUS = 128
LAYERS_ALL = 512
NX = 512
NY = 4096


def with_ends(array, own_key, smallest, largest):
    index_at = [jax.random.randint(jax.random.fold_in(own_key, axis), (), 0, length) for axis, length in enumerate(array.shape)]
    longest = array.shape.index(max(array.shape))
    beside = index_at[:longest] + [(index_at[longest] + 1) % array.shape[longest]] + index_at[longest + 1:]
    return array.at[tuple(index_at)].set(smallest).at[tuple(beside)].set(largest)


def level_of(own_key, dims, cuts, least, top_value):
    def one(dim, blocks):
        heights = jax.random.uniform(jax.random.fold_in(jax.random.fold_in(own_key, 6), dim), (blocks,), jnp.float32, least / len(cuts), top_value / len(cuts))
        return jnp.repeat(jnp.exp(heights), dims[dim] // blocks).reshape((-1,) + (1,) * (len(dims) - dim - 1))

    gain = one(*cuts[0])
    for cut in cuts[1:]:
        gain = gain * one(*cut)
    return gain


def centred(rng, shape, deviation, bound, cuts=(), held_as=jnp.bfloat16):
    loudness = level_of(rng, shape, cuts, -0.22, 0.18) if cuts else 1.0
    array = jax.random.normal(rng, shape, jnp.float32) * deviation * loudness
    return jnp.minimum(jnp.maximum(array, -bound), bound).astype(held_as)


def setup_inputs(seed: int = 0) -> dict:
    key_list = jax.random.split(jax.random.key(seed), 5)
    density = centred(key_list[0], (LAYERS, NX, NY), 1.0, 6.0, ((1, 2), (2, 16)), jnp.float32)
    observed = centred(key_list[1], (NX, NY), 1.0, 6.0, ((0, 2), (1, 16)), jnp.float32)
    stations = with_ends((jax.random.randint(key_list[2], (NX, NY), 0, 2) < 1).astype(jnp.int32), jax.random.fold_in(key_list[2], 1), 0, 1)
    layer_index = jax.random.randint(key_list[3], (LAYERS,), 0, LAYERS_ALL).astype(jnp.int32)
    return {"density": density, "observed": observed, "stations": stations, "layer_index": layer_index}


def signed_offsets(length):
    ticks = jnp.arange(length, dtype=jnp.int32)
    return jnp.where(ticks <= RADIUS, ticks, ticks - length).astype(jnp.float32)

def kernel_grid(index, rows, cols):
    first = signed_offsets(rows)
    second = signed_offsets(cols)
    depth = RADIUS * (0.375 + index.astype(jnp.float32) / LAYERS_ALL)
    square = first[:, None] ** 2 + second[None, :] ** 2 + depth * depth
    value = depth * depth / (square * jnp.sqrt(square))
    inside = (jnp.abs(first) <= RADIUS)[:, None] & (jnp.abs(second) <= RADIUS)[None, :]
    return jnp.where(inside, value, jnp.zeros_like(value))

def convolve(kernel_hat, field, rows, cols):
    padded = jnp.pad(field, RADIUS)
    whole = jnp.fft.irfft2(kernel_hat * jnp.fft.rfft2(padded), s=(rows, cols))
    return whole[RADIUS:RADIUS + NX, RADIUS:RADIUS + NY].astype(jnp.float32)

def reference(density, observed, stations, layer_index):
    rows = NX + 2 * RADIUS
    cols = NY + 2 * RADIUS
    spectra = [jnp.fft.rfft2(kernel_grid(layer_index[layer], rows, cols)) for layer in range(LAYERS)]
    predicted = jnp.zeros((NX, NY), jnp.float32)
    for layer in range(LAYERS):
        predicted = predicted + convolve(spectra[layer], density[layer], rows, cols)
    residual = stations.astype(jnp.float32) * (predicted - observed)
    gradient = jnp.stack([convolve(spectra[layer], residual, rows, cols) for layer in range(LAYERS)])
    return (predicted, residual, gradient)
```

```python
import functools
import math

import jax
import jax.numpy as jnp
import ml_dtypes
import numpy as np
from jax import lax
from jax.experimental import pallas as pl
from jax.experimental.pallas import tpu as pltpu
from jax.sharding import PartitionSpec as P

RADIUS = 128
LAYERS_ALL = 512

F32 = jnp.float32
BF16 = jnp.bfloat16


def halves(table):
    table = table.astype(np.float32)
    high = table.astype(ml_dtypes.bfloat16)
    low = (table - high.astype(np.float32)).astype(ml_dtypes.bfloat16)
    return [high, low]


@functools.lru_cache(maxsize=None)
def tables(tile):
    length = 2 * tile
    half = tile // 2
    ticks = np.arange(tile)
    even = 2 * np.arange(half)
    odd = even + 1

    def angles(freqs):
        return (freqs[:, None] * ticks[None, :] % length) * (2.0 * math.pi / length)

    middle = even.copy()
    middle[0] = tile
    even_sin = np.sin(angles(even))
    even_sin[0] = np.cos(angles(middle))[0]
    basis = np.concatenate([np.cos(angles(even)), even_sin, np.cos(angles(odd)), np.sin(angles(odd))])
    fold = np.where(ticks == 0, 1.0, 2.0) * (ticks <= RADIUS)
    freqs = np.concatenate([even, middle, odd])
    weights = np.where((freqs == 0) | (freqs == tile), 1.0, 2.0) / length
    sides = np.cos(angles(freqs)) * fold[None, :] * weights[:, None]
    return halves(basis) + halves(basis.T) + halves(sides) + halves(sides.T)


def parts(value):
    high = value.astype(BF16)
    return high, (value - high.astype(F32)).astype(BF16)


def product(left, right):
    def dot(a, b):
        return jnp.dot(a, b, preferred_element_type=F32)

    return dot(left[0], right[0]) + (dot(left[0], right[1]) + dot(left[1], right[0]))


def pair(refs, *index):
    return refs[0][index], refs[1][index]


def spectrum(index, sides, sides_t, tile):
    rows = lax.broadcasted_iota(jnp.int32, (tile, tile), 0)
    cols = lax.broadcasted_iota(jnp.int32, (tile, tile), 1)
    depth = RADIUS * (0.375 + index.astype(F32) / LAYERS_ALL)
    depth2 = depth * depth
    square = (rows * rows + cols * cols).astype(F32) + depth2
    value = depth2 / (square * jnp.sqrt(square))
    first = product(parts(value), pair(sides_t, slice(None), slice(None)))
    return product(pair(sides, slice(None), slice(None)), parts(first))


def group(block, half):
    return slice(min(block, 2) * half, (min(block, 2) + 1) * half)


def forward_kernel(phases, tile, layers, scalars, density, *refs):
    basis, basis_t, sides, sides_t = refs[0:2], refs[2:4], refs[4:6], refs[6:8]
    spectra, own = refs[8:10]
    sends = refs[10:-3]
    total, spill_rows, spill_both = refs[-3:]
    half = tile // 2
    everything = slice(None)
    for layer in range(layers):
        spec = spectrum(scalars[2 + layer], sides, sides_t, tile)
        spectra[layer] = spec
        first = product(parts(density[layer]), pair(basis_t, everything, everything))
        field = product(pair(basis, everything, everything), parts(first))
        for a in range(4):
            for b in range(4):
                rows, cols = slice(a * half, (a + 1) * half), slice(b * half, (b + 1) * half)
                term = spec[group(a, half), group(b, half)] * field[rows, cols]
                total[rows, cols] = term if layer == 0 else total[rows, cols] + term
    low, high = slice(0, tile), slice(tile, 2 * tile)
    even = product(pair(basis_t, everything, low), parts(total[low, :]))
    odd = product(pair(basis_t, everything, high), parts(total[high, :]))
    plus, minus = even + odd, even - odd

    def columns(value):
        first = product(parts(value[:, low]), pair(basis, low, everything))
        second = product(parts(value[:, high]), pair(basis, high, everything))
        return first + second, first - second

    own_value, spill_cols_value = columns(plus)
    own[...] = own_value
    total[low, low] = spill_cols_value
    spill_rows[...], spill_both[...] = columns(minus)
    for ref, (px, py) in zip(sends, phases):
        if py is None:
            ref[...] = spill_rows[pl.ds(pl.multiple_of(scalars_off(scalars, 0, px), RADIUS), RADIUS), :]
        elif px is None:
            ref[...] = total[low, pl.ds(pl.multiple_of(scalars_off(scalars, 1, py), RADIUS), RADIUS)]
        else:
            ref[...] = spill_both[
                pl.ds(pl.multiple_of(scalars_off(scalars, 0, px), RADIUS), RADIUS),
                pl.ds(pl.multiple_of(scalars_off(scalars, 1, py), RADIUS), RADIUS),
            ]


def scalars_off(scalars, axis, phase):
    return jnp.where(scalars[axis] == phase, 0, RADIUS)


def own_slice(scalars, axis, phase):
    return pl.ds(pl.multiple_of(RADIUS - scalars_off(scalars, axis, phase), RADIUS), RADIUS)


def halo_slice(scalars, axis, phase):
    return pl.ds(pl.multiple_of(scalars_off(scalars, axis, phase), RADIUS), RADIUS)


def residual_kernel(phases, scalars, own, observed, stations, *refs):
    count = len(phases)
    received, (predicted, residual), sends = refs[:count], refs[count : count + 2], refs[count + 2 :]
    predicted[...] = own[...]

    def at(px, py):
        rows = slice(None) if px is None else own_slice(scalars, 0, px)
        cols = slice(None) if py is None else own_slice(scalars, 1, py)
        return rows, cols

    for ref, (px, py) in zip(received, phases):
        index = at(px, py)
        predicted[index] += ref[...]
    residual[...] = stations[...].astype(F32) * (predicted[...] - observed[...])
    for ref, (px, py) in zip(sends, phases):
        ref[...] = residual[at(px, py)]


def adjoint_kernel(phases, tile, layers, scalars, residual, spectra, *refs):
    count = len(phases)
    received = refs[:count]
    basis, basis_t = refs[count : count + 2], refs[count + 2 : count + 4]
    gradient, x01, x10, x11, held = refs[count + 4 :]
    half = tile // 2
    everything = slice(None)
    if len(phases) < 8:
        x01[...] = jnp.zeros_like(x01)
        x10[...] = jnp.zeros_like(x10)
        x11[...] = jnp.zeros_like(x11)
    for ref, (px, py) in zip(received, phases):
        if py is None:
            x10[halo_slice(scalars, 0, px), :] = ref[...]
        elif px is None:
            x01[:, halo_slice(scalars, 1, py)] = ref[...]
        else:
            x11[halo_slice(scalars, 0, px), halo_slice(scalars, 1, py)] = ref[...]
    low, high = slice(0, tile), slice(tile, 2 * tile)
    up_even, up_odd = residual[...] + x01[...], residual[...] - x01[...]
    down_even, down_odd = x10[...] + x11[...], x10[...] - x11[...]

    def rows_of(even, odd, which):
        first = product(parts(even), pair(basis_t, everything, low))
        second = product(parts(odd), pair(basis_t, everything, high))
        held[which, low] = product(pair(basis, which, everything), parts(first))
        held[which, high] = product(pair(basis, which, everything), parts(second))

    rows_of(up_even + down_even, up_odd + down_odd, low)
    rows_of(up_even - down_even, up_odd - down_odd, high)
    for layer in range(layers):

        def scaled(a):
            rows = slice(a * half, (a + 1) * half)
            return jnp.concatenate(
                [
                    spectra[layer, group(a, half), group(b, half)] * held[rows, b * half : (b + 1) * half]
                    for b in range(4)
                ],
                axis=1,
            )

        even = jnp.concatenate([scaled(0), scaled(1)], axis=0)
        odd = jnp.concatenate([scaled(2), scaled(3)], axis=0)
        mid = product(pair(basis_t, everything, low), parts(even)) + product(
            pair(basis_t, everything, high), parts(odd)
        )
        gradient[layer] = product(parts(mid[:, low]), pair(basis, low, everything)) + product(
            parts(mid[:, high]), pair(basis, high, everything)
        )


def partner(index, phase):
    return index + 1 if index % 2 == phase else index - 1


def exchange(values, phases):
    nx, ny = lax.axis_size("gx"), lax.axis_size("gy")
    received = []
    for value, (px, py) in zip(values, phases):
        links = []
        for i in range(nx):
            for j in range(ny):
                x = i if px is None else partner(i, px)
                y = j if py is None else partner(j, py)
                if 0 <= x < nx and 0 <= y < ny:
                    links.append((i * ny + j, x * ny + y))
        received.append(lax.ppermute(value, ("gx", "gy"), links))
    return received


def body(density, observed, stations, layer_index):
    layers, tile = density.shape[0], density.shape[1]
    nx, ny = lax.axis_size("gx"), lax.axis_size("gy")
    xs = [phase for phase in range(2) if nx > 1 + phase]
    ys = [phase for phase in range(2) if ny > 1 + phase]
    phases = [(px, None) for px in xs] + [(None, py) for py in ys] + [(px, py) for px in xs for py in ys]

    def strip(px, py):
        shape = (tile if px is None else RADIUS, tile if py is None else RADIUS)
        return jax.ShapeDtypeStruct(shape, F32)

    strips = [strip(*phase) for phase in phases]
    consts = [jnp.asarray(table) for table in tables(tile)]
    scalars = jnp.concatenate(
        [jnp.stack([lax.axis_index("gx") % 2, lax.axis_index("gy") % 2]).astype(jnp.int32), layer_index]
    )
    smem = pl.BlockSpec(memory_space=pltpu.SMEM)
    vmem = pl.BlockSpec(memory_space=pltpu.VMEM)
    square = jax.ShapeDtypeStruct((tile, tile), F32)
    groups = 3 * (tile // 2)

    out = pl.pallas_call(
        functools.partial(forward_kernel, phases, tile, layers),
        out_shape=[jax.ShapeDtypeStruct((layers, groups, groups), F32), square] + strips,
        in_specs=[smem] + [vmem] * (1 + len(consts)),
        out_specs=[vmem] * (2 + len(strips)),
        scratch_shapes=[
            pltpu.VMEM((2 * tile, 2 * tile), F32),
            pltpu.VMEM((tile, tile), F32),
            pltpu.VMEM((tile, tile), F32),
        ],
        name="forward",
    )(scalars, density, *consts)
    spectra, own, sends = out[0], out[1], out[2:]
    received = exchange(sends, phases)
    out = pl.pallas_call(
        functools.partial(residual_kernel, phases),
        out_shape=[square, square] + strips,
        in_specs=[smem] + [vmem] * (3 + len(strips)),
        out_specs=[vmem] * (2 + len(strips)),
        name="residual",
    )(scalars, own, observed, stations, *received)
    predicted, residual, sends = out[0], out[1], out[2:]
    received = exchange(sends, phases)
    gradient = pl.pallas_call(
        functools.partial(adjoint_kernel, phases, tile, layers),
        out_shape=jax.ShapeDtypeStruct((layers, tile, tile), F32),
        in_specs=[smem] + [vmem] * (2 + len(strips) + 4),
        out_specs=vmem,
        scratch_shapes=[
            pltpu.VMEM((tile, tile), F32),
            pltpu.VMEM((tile, tile), F32),
            pltpu.VMEM((tile, tile), F32),
            pltpu.VMEM((2 * tile, 2 * tile), F32),
        ],
        name="adjoint",
    )(scalars, residual, spectra, *received, *consts[:4])
    return predicted, residual, gradient


def solution(mesh):
    in_specs = (P(None, "gx", "gy"), P("gx", "gy"), P("gx", "gy"), P())
    out_specs = (P("gx", "gy"), P("gx", "gy"), P(None, "gx", "gy"))
    return jax.shard_map(body, mesh=mesh, in_specs=in_specs, out_specs=out_specs, check_vma=False)
```

```python
import functools
import math

import jax
import jax.numpy as jnp
import ml_dtypes
import numpy as np
from jax import lax
from jax.experimental import pallas as pl
from jax.experimental.pallas import tpu as pltpu
from jax.sharding import PartitionSpec as P

RADIUS = 128
LAYERS_ALL = 512

F32 = jnp.float32
BF16 = jnp.bfloat16
PARAMS = pltpu.CompilerParams(vmem_limit_bytes=24 * 2**20)


def halves(table):
    table = table.astype(np.float32)
    high = table.astype(ml_dtypes.bfloat16)
    low = (table - high.astype(np.float32)).astype(ml_dtypes.bfloat16)
    return [high, low]


@functools.lru_cache(maxsize=None)
def tables(tile):
    length = 2 * tile
    half = tile // 2
    ticks = np.arange(tile)
    even = 2 * np.arange(half)
    odd = even + 1

    def angles(freqs):
        return (freqs[:, None] * ticks[None, :] % length) * (2.0 * math.pi / length)

    middle = even.copy()
    middle[0] = tile
    even_sin = np.sin(angles(even))
    even_sin[0] = np.cos(angles(middle))[0]
    basis = np.concatenate([np.cos(angles(even)), even_sin, np.cos(angles(odd)), np.sin(angles(odd))])
    fold = np.where(ticks == 0, 1.0, 2.0) * (ticks <= RADIUS)
    freqs = np.concatenate([even, middle, odd])
    weights = np.where((freqs == 0) | (freqs == tile), 1.0, 2.0) / length
    sides = np.cos(angles(freqs)) * fold[None, :] * weights[:, None]
    return halves(basis) + halves(basis.T) + halves(sides) + halves(sides.T)


def parts(value):
    high = value.astype(BF16)
    return high, (value - high.astype(F32)).astype(BF16)


def product(left, right):
    def dot(a, b):
        return jnp.dot(a, b, preferred_element_type=F32)

    return dot(left[0], right[0]) + (dot(left[0], right[1]) + dot(left[1], right[0]))


def pair(refs, *index):
    return refs[0][index], refs[1][index]


def side(axis, phase):
    return jnp.where((lax.axis_index(axis) & 1) == phase, 0, RADIUS)


def halo(axis, phase):
    return pl.ds(pl.multiple_of(side(axis, phase), RADIUS), RADIUS)


def edge(axis, phase):
    return pl.ds(pl.multiple_of(RADIUS - side(axis, phase), RADIUS), RADIUS)


def group(block, half):
    return slice(min(block, 2) * half, (min(block, 2) + 1) * half)


ALL = slice(None)


def spectrum_kernel(tile, layers, index_source, *refs):
    sources, spectra, held, index, sems = refs[:4], refs[4], refs[5:9], refs[9], refs[10]
    copies = [pltpu.make_async_copy(sources[k], held[k], sems.at[k]) for k in range(4)]
    copies.append(pltpu.make_async_copy(index_source, index, sems.at[4]))
    for copy in reversed(copies):
        copy.start()
    span = RADIUS + 8
    rows = lax.broadcasted_iota(jnp.int32, (span, tile), 0)
    cols = lax.broadcasted_iota(jnp.int32, (span, tile), 1)
    offsets = (rows * rows + cols * cols).astype(F32)
    copies[4].wait()
    values = []
    for layer in range(layers):
        depth = RADIUS * (0.375 + index[layer].astype(F32) / LAYERS_ALL)
        square = offsets + depth * depth
        values.append(depth * depth / (square * jnp.sqrt(square)))
    copies[2].wait()
    copies[3].wait()
    first = product(parts(jnp.concatenate(values, axis=0)), pair(held[2:], ALL, ALL))
    copies[0].wait()
    copies[1].wait()
    rest = jnp.zeros((tile - span, first.shape[1]), F32)
    for layer in range(layers):
        own = jnp.concatenate([first[layer * span : (layer + 1) * span], rest], axis=0)
        spectra[layer] = product(pair(held[:2], ALL, ALL), parts(own))


def forward_kernel(xs, ys, tile, layers, density, spectra, *refs):
    count = len(ys)
    received, basis, basis_t = refs[:count], refs[count : count + 2], refs[count + 2 : count + 4]
    own, spill = refs[count + 4 : count + 6]
    sends, (wrapped, total) = refs[count + 6 : -2], refs[-2:]
    half = tile // 2
    low, high = slice(0, tile), slice(tile, 2 * tile)
    if count < 2:
        wrapped[...] = jnp.zeros_like(wrapped)
    for ref, phase in zip(received, ys):
        for layer in range(layers):
            wrapped[layer * tile : (layer + 1) * tile, halo("gy", phase)] = ref[layer]
    field = jnp.concatenate([density[layer] for layer in range(layers)], axis=0)
    behind = wrapped[...]
    even = product(parts(field + behind), pair(basis_t, ALL, low))
    odd = product(parts(field - behind), pair(basis_t, ALL, high))
    for layer in range(layers):
        rows = slice(layer * tile, (layer + 1) * tile)
        both = jnp.concatenate([even[rows], odd[rows]], axis=1)
        value = product(pair(basis, ALL, ALL), parts(both))
        for a in range(4):
            for b in range(4):
                place = slice(a * half, (a + 1) * half), slice(b * half, (b + 1) * half)
                term = spectra[layer, group(a, half), group(b, half)] * value[place]
                total[place] = term if layer == 0 else total[place] + term
    mixed = product(parts(total[:, low]), pair(basis, low, ALL)) + product(
        parts(total[:, high]), pair(basis, high, ALL)
    )
    even = product(pair(basis_t, ALL, low), parts(mixed[low]))
    odd = product(pair(basis_t, ALL, high), parts(mixed[high]))
    own[...] = even + odd
    spill[...] = even - odd
    for ref, phase in zip(sends, xs):
        ref[:RADIUS] = own[edge("gx", phase)]
        ref[RADIUS:] = spill[halo("gx", phase)]


def residual_kernel(xs, ys, tile, own, spill, observed, stations, *refs):
    count = len(xs)
    received, strips = refs[:count], refs[count : 2 * count]
    predicted, residual, behind = refs[2 * count : 2 * count + 3]
    sends = refs[2 * count + 3 :]
    predicted[...] = own[...]
    if count < 2:
        behind[...] = jnp.zeros_like(behind)
    for ref, strip, phase in zip(received, strips, xs):
        predicted[edge("gx", phase)] += ref[RADIUS:]
        rows = halo("gx", phase)
        behind[rows] = strip[1] * (spill[rows] + ref[:RADIUS] - strip[0])
    residual[...] = stations[...].astype(F32) * (predicted[...] - observed[...])
    for ref, phase in zip(sends, ys):
        cols = edge("gy", phase)
        ref[:tile] = residual[:, cols]
        for k, other in enumerate(xs):
            start = tile + k * RADIUS
            ref[start : start + RADIUS] = behind[halo("gx", other), cols]


def adjoint_kernel(xs, ys, tile, layers, predicted, residual, behind, spectra, *refs):
    count = len(ys)
    received, basis, basis_t = refs[:count], refs[count : count + 2], refs[count + 2 : count + 4]
    predicted_out, residual_out, gradient = refs[count + 4 : count + 7]
    across, corner, held, result, sems = refs[count + 7 :]
    half = tile // 2
    low, high = slice(0, tile), slice(tile, 2 * tile)
    copies = [
        pltpu.make_async_copy(predicted, predicted_out, sems.at[0]),
        pltpu.make_async_copy(residual, residual_out, sems.at[1]),
    ]
    for copy in copies:
        copy.start()
    if count < 2:
        across[...] = jnp.zeros_like(across)
    if count < 2 or len(xs) < 2:
        corner[...] = jnp.zeros_like(corner)
    for ref, phase in zip(received, ys):
        cols = halo("gy", phase)
        across[:, cols] = ref[:tile]
        for k, other in enumerate(xs):
            start = tile + k * RADIUS
            corner[halo("gx", other), cols] = ref[start : start + RADIUS]
    up_even, up_odd = residual[...] + across[...], residual[...] - across[...]
    down_even, down_odd = behind[...] + corner[...], behind[...] - corner[...]
    even = jnp.concatenate([up_even + down_even, up_even - down_even], axis=0)
    odd = jnp.concatenate([up_odd + down_odd, up_odd - down_odd], axis=0)
    even = product(parts(even), pair(basis_t, ALL, low))
    odd = product(parts(odd), pair(basis_t, ALL, high))
    for rows in (low, high):
        both = jnp.concatenate([even[rows], odd[rows]], axis=1)
        held[rows] = product(pair(basis, rows, ALL), parts(both))
    for layer in range(layers):

        def scaled(a):
            rows = slice(a * half, (a + 1) * half)
            return jnp.concatenate(
                [
                    spectra[layer, group(a, half), group(b, half)] * held[rows, b * half : (b + 1) * half]
                    for b in range(4)
                ],
                axis=1,
            )

        scaled_rows = [scaled(a) for a in range(4)]
        whole = jnp.concatenate(scaled_rows, axis=0)
        mixed = product(parts(whole[:, low]), pair(basis, low, ALL)) + product(
            parts(whole[:, high]), pair(basis, high, ALL)
        )
        result[layer] = product(pair(basis_t, ALL, low), parts(mixed[low])) + product(
            pair(basis_t, ALL, high), parts(mixed[high])
        )
        copies.append(pltpu.make_async_copy(result.at[layer], gradient.at[layer], sems.at[2 + layer]))
        copies[-1].start()
    for copy in copies:
        copy.wait()


def partner(index, phase):
    return index + 1 if index % 2 == phase else index - 1


def swap(value, axis, phase):
    count = lax.axis_size(axis)
    links = [(i, partner(i, phase)) for i in range(count)]
    return lax.ppermute(value, axis, [link for link in links if 0 <= link[1] < count])


def in_hbm(value):
    return pltpu.with_memory_space_constraint(value, pltpu.HBM)


def phases(axis):
    return [phase for phase in (1, 0) if lax.axis_size(axis) > 1 + phase]


def cost(units, tile):
    flops = int(units * 6 * tile**3)
    return pl.CostEstimate(flops=flops, bytes_accessed=tile * tile * 16, transcendentals=0)


def body(density, observed, stations, layer_index):
    layers, tile = density.shape[0], density.shape[1]
    xs, ys = phases("gx"), phases("gy")
    groups = 3 * (tile // 2)
    consts = [jnp.asarray(table) for table in tables(tile)]
    basis, sides = consts[:4], consts[4:]
    vmem = pl.BlockSpec(memory_space=pltpu.VMEM)
    hbm = pl.BlockSpec(memory_space=pltpu.HBM)

    def array(*shape):
        return jax.ShapeDtypeStruct(shape, F32)

    def cols_of(phase):
        upper = (lax.axis_index("gy") & 1) == phase
        return jnp.where(upper, density[..., tile - RADIUS :], density[..., :RADIUS])

    def rows_of(phase):
        upper = (lax.axis_index("gx") & 1) == phase
        both = jnp.stack([observed, stations.astype(F32)])
        return jnp.where(upper, both[:, tile - RADIUS :], both[:, :RADIUS])

    density_halos = [swap(cols_of(phase), "gy", phase) for phase in ys]
    strips = [swap(rows_of(phase), "gx", phase) for phase in xs]
    spectra = pl.pallas_call(
        functools.partial(spectrum_kernel, tile, layers),
        out_shape=array(layers, groups, groups),
        in_specs=[hbm] * 5,
        out_specs=vmem,
        scratch_shapes=[pltpu.VMEM(table.shape, BF16) for table in sides]
        + [pltpu.SMEM((layers,), jnp.int32), pltpu.SemaphoreType.DMA((5,))],
        compiler_params=PARAMS,
        cost_estimate=cost(8, tile),
        name="spectrum",
    )(*[in_hbm(value) for value in (layer_index, *sides)])
    out = pl.pallas_call(
        functools.partial(forward_kernel, xs, ys, tile, layers),
        out_shape=[array(tile, tile)] * (2 + len(xs)),
        in_specs=[vmem] * (6 + len(ys)),
        out_specs=[vmem] * (2 + len(xs)),
        scratch_shapes=[pltpu.VMEM((layers * tile, tile), F32), pltpu.VMEM((2 * tile, 2 * tile), F32)],
        compiler_params=PARAMS,
        cost_estimate=cost(18, tile),
        name="forward",
    )(density, spectra, *density_halos, *basis)
    own, spill, sends = out[0], out[1], out[2:]
    received = [swap(value, "gx", phase) for value, phase in zip(sends, xs)]
    tall = tile + RADIUS * len(xs)
    out = pl.pallas_call(
        functools.partial(residual_kernel, xs, ys, tile),
        out_shape=[array(tile, tile)] * 3 + [array(tall, RADIUS)] * len(ys),
        in_specs=[vmem] * (4 + 2 * len(xs)),
        out_specs=[vmem] * (3 + len(ys)),
        compiler_params=PARAMS,
        cost_estimate=cost(1, tile),
        name="residual",
    )(own, spill, observed, stations, *received, *strips)
    predicted, residual, behind, sends = out[0], out[1], out[2], out[3:]
    received = [swap(value, "gy", phase) for value, phase in zip(sends, ys)]
    return pl.pallas_call(
        functools.partial(adjoint_kernel, xs, ys, tile, layers),
        out_shape=[array(tile, tile), array(tile, tile), array(layers, tile, tile)],
        in_specs=[vmem] * (8 + len(ys)),
        out_specs=[hbm] * 3,
        scratch_shapes=[
            pltpu.VMEM((tile, tile), F32),
            pltpu.VMEM((tile, tile), F32),
            pltpu.VMEM((2 * tile, 2 * tile), F32),
            pltpu.VMEM((layers, tile, tile), F32),
            pltpu.SemaphoreType.DMA((2 + layers,)),
        ],
        compiler_params=PARAMS,
        cost_estimate=cost(20, tile),
        name="adjoint",
    )(predicted, residual, behind, spectra, *received, *basis)


def solution(mesh):
    in_specs = (P(None, "gx", "gy"), P("gx", "gy"), P("gx", "gy"), P())
    out_specs = (P("gx", "gy"), P("gx", "gy"), P(None, "gx", "gy"))
    return jax.shard_map(body, mesh=mesh, in_specs=in_specs, out_specs=out_specs, check_vma=False)
```

```python
import functools
import itertools
import math

import jax
import jax.numpy as jnp
import ml_dtypes
import numpy as np
from jax import lax
from jax.experimental import pallas as pl
from jax.experimental.pallas import tpu as pltpu
from jax.sharding import PartitionSpec as P


RADIUS = 128
LAYERS_ALL = 512

F32 = jnp.float32
BF16 = jnp.bfloat16
PARAMS = pltpu.CompilerParams(vmem_limit_bytes=24 * 2**20)


def halves(table):
    table = table.astype(np.float32)
    high = table.astype(ml_dtypes.bfloat16)
    low = (table - high.astype(np.float32)).astype(ml_dtypes.bfloat16)
    return [high, low]


@functools.lru_cache(maxsize=None)
def tables(tile):
    length = 2 * tile
    half = tile // 2
    ticks = np.arange(tile)
    even = 2 * np.arange(half)
    odd = even + 1

    def angles(freqs):
        return (freqs[:, None] * ticks[None, :] % length) * (2.0 * math.pi / length)

    middle = even.copy()
    middle[0] = tile
    even_sin = np.sin(angles(even))
    even_sin[0] = np.cos(angles(middle))[0]
    basis = np.concatenate([np.cos(angles(even)), even_sin, np.cos(angles(odd)), np.sin(angles(odd))])
    fold = np.where(ticks == 0, 1.0, 2.0) * (ticks <= RADIUS)
    freqs = np.concatenate([even, middle, odd])
    weights = np.where((freqs == 0) | (freqs == tile), 1.0, 2.0) / length
    sides = np.cos(angles(freqs)) * fold[None, :] * weights[:, None]
    return halves(basis) + halves(basis.T) + halves(sides) + halves(sides.T)


def parts(value):
    high = value.astype(BF16)
    return high, (value - high.astype(F32)).astype(BF16)


def product(left, right):
    def dot(a, b):
        return jnp.dot(a, b, preferred_element_type=F32)

    return dot(left[0], right[0]) + (dot(left[0], right[1]) + dot(left[1], right[0]))


def pair(refs, *index):
    return refs[0][index], refs[1][index]


def side(axis, phase):
    return jnp.where((lax.axis_index(axis) & 1) == phase, 0, RADIUS)


def halo(axis, phase):
    return pl.ds(pl.multiple_of(side(axis, phase), RADIUS), RADIUS)


def edge(axis, phase):
    return pl.ds(pl.multiple_of(RADIUS - side(axis, phase), RADIUS), RADIUS)


def group(block, half):
    return slice(min(block, 2) * half, (min(block, 2) + 1) * half)


ALL = slice(None)


def spectrum_kernel(tile, layers, index_source, *refs):
    sources, spectra, held, index, sems = refs[:4], refs[4], refs[5:9], refs[9], refs[10]
    copies = [pltpu.make_async_copy(sources[k], held[k], sems.at[k]) for k in range(4)]
    copies.append(pltpu.make_async_copy(index_source, index, sems.at[4]))
    for copy in reversed(copies):
        copy.start()
    span = RADIUS + 8
    rows = lax.broadcasted_iota(jnp.int32, (span, tile), 0)
    cols = lax.broadcasted_iota(jnp.int32, (span, tile), 1)
    offsets = (rows * rows + cols * cols).astype(F32)
    copies[4].wait()
    values = []
    for layer in range(layers):
        depth = RADIUS * (0.375 + index[layer].astype(F32) / LAYERS_ALL)
        square = offsets + depth * depth
        values.append(depth * depth / (square * jnp.sqrt(square)))
    copies[2].wait()
    copies[3].wait()
    first = product(parts(jnp.concatenate(values, axis=0)), pair(held[2:], ALL, ALL))
    copies[0].wait()
    copies[1].wait()
    rest = jnp.zeros((tile - span, first.shape[1]), F32)
    for layer in range(layers):
        own = jnp.concatenate([first[layer * span : (layer + 1) * span], rest], axis=0)
        spectra[layer] = product(pair(held[:2], ALL, ALL), parts(own))


def forward_kernel(xs, ys, early, tile, layers, density, spectra, observed, stations, *refs):
    received, refs = refs[: len(ys)], refs[len(ys) :]
    basis, basis_t, (own, spill), refs = refs[:2], refs[2:4], refs[4:6], refs[6:]
    sends, firsts, (wrapped, total) = refs[: 2 * len(xs)], refs[2 * len(xs) : -2], refs[-2:]
    half = tile // 2
    low, high = slice(0, tile), slice(tile, 2 * tile)
    if len(ys) < 2:
        wrapped[...] = jnp.zeros_like(wrapped)
    for ref, phase in zip(received, ys):
        for layer in range(layers):
            wrapped[layer * tile : (layer + 1) * tile, halo("gy", phase)] = ref[layer]
    field = jnp.concatenate([density[layer] for layer in range(layers)], axis=0)
    behind = wrapped[...]
    even = product(parts(field + behind), pair(basis_t, ALL, low))
    odd = product(parts(field - behind), pair(basis_t, ALL, high))
    for layer in range(layers):
        rows = slice(layer * tile, (layer + 1) * tile)
        both = jnp.concatenate([even[rows], odd[rows]], axis=1)
        value = product(pair(basis, ALL, ALL), parts(both))
        for a in range(4):
            for b in range(4):
                place = slice(a * half, (a + 1) * half), slice(b * half, (b + 1) * half)
                term = spectra[layer, group(a, half), group(b, half)] * value[place]
                total[place] = term if layer == 0 else total[place] + term
    mixed = product(parts(total[:, low]), pair(basis, low, ALL)) + product(
        parts(total[:, high]), pair(basis, high, ALL)
    )
    even = product(pair(basis_t, ALL, low), parts(mixed[low]))
    odd = product(pair(basis_t, ALL, high), parts(mixed[high]))
    own[...] = even + odd
    spill[...] = even - odd
    for k, (phase, other) in enumerate(itertools.product(xs, (1, 0))):
        sends[k][:RADIUS] = spill[halo("gx", phase), edge("gy", other)]
        sends[k][RADIUS:] = own[edge("gx", phase), edge("gy", other)]
    if early:
        place = halo("gx", xs[0]), edge("gy", 1)
        firsts[0][...] = stations[place].astype(F32) * (own[place] - observed[place])


def side_kernel(xs, early, other, tile, own, spill, observed, stations, *refs):
    count = len(xs)
    received, strips, refs = refs[:count], refs[count : 2 * count], refs[2 * count :]
    (predicted, residual, behind), sends = refs[:3], refs[3:]
    cols = edge("gy", other)
    predicted[...] = own[:, cols]
    if count < 2:
        behind[...] = jnp.zeros_like(behind)
    for ref, strip, phase in zip(received, strips, xs):
        predicted[edge("gx", phase)] += ref[:RADIUS]
        rows = halo("gx", phase)
        behind[rows] = strip[1, :, cols] * (spill[rows, cols] + ref[RADIUS:] - strip[0, :, cols])
    residual[...] = stations[:, cols].astype(F32) * (predicted[...] - observed[:, cols])
    for ref in sends:
        if early and other:
            ref[:RADIUS] = residual[edge("gx", xs[0])]
        else:
            ref[:tile] = residual[...]
        for k, phase in enumerate(xs):
            start = ref.shape[0] + (k - count) * RADIUS
            ref[start : start + RADIUS] = behind[halo("gx", phase)]


def adjoint_kernel(xs, ys, early, tile, layers, spectra, *refs):
    halves, firsts, refs = (refs[:3], refs[3:6]), refs[6 : 6 + early], refs[6 + early :]
    strips, basis, basis_t, refs = refs[: len(ys)], refs[len(ys) :][:2], refs[len(ys) :][2:4], refs[len(ys) + 4 :]
    predicted_out, residual_out, gradient = refs[:3]
    residual, behind, across, corner, held, result, sems = refs[3:]
    half = tile // 2
    low, high = slice(0, tile), slice(tile, 2 * tile)
    copies = []
    for k, other in enumerate((1, 0)):
        cols = edge("gy", other)
        copies.append(pltpu.make_async_copy(halves[k][0], predicted_out.at[:, cols], sems.at[2 * k]))
        copies.append(pltpu.make_async_copy(halves[k][1], residual_out.at[:, cols], sems.at[2 * k + 1]))
    for copy in copies:
        copy.start()
    for k, other in enumerate((1, 0)):
        residual[:, edge("gy", other)] = halves[k][1][...]
        behind[:, edge("gy", other)] = halves[k][2][...]
    if len(ys) < 2:
        across[...] = jnp.zeros_like(across)
    if len(ys) < 2 or len(xs) < 2:
        corner[...] = jnp.zeros_like(corner)
    for ref, phase in zip(strips, ys):
        cols = halo("gy", phase)
        if early and phase:
            across[halo("gx", xs[0]), cols] = firsts[0][...]
            across[edge("gx", xs[0]), cols] = ref[:RADIUS]
        else:
            across[:, cols] = ref[:tile]
        for k, other in enumerate(xs):
            start = ref.shape[0] + (k - len(xs)) * RADIUS
            corner[halo("gx", other), cols] = ref[start : start + RADIUS]
    up_even, up_odd = residual[...] + across[...], residual[...] - across[...]
    down_even, down_odd = behind[...] + corner[...], behind[...] - corner[...]
    even = jnp.concatenate([up_even + down_even, up_even - down_even], axis=0)
    odd = jnp.concatenate([up_odd + down_odd, up_odd - down_odd], axis=0)
    even = product(parts(even), pair(basis_t, ALL, low))
    odd = product(parts(odd), pair(basis_t, ALL, high))
    for rows in (low, high):
        both = jnp.concatenate([even[rows], odd[rows]], axis=1)
        held[rows] = product(pair(basis, rows, ALL), parts(both))
    for layer in range(layers):

        def scaled(a):
            rows = slice(a * half, (a + 1) * half)
            return jnp.concatenate(
                [
                    spectra[layer, group(a, half), group(b, half)] * held[rows, b * half : (b + 1) * half]
                    for b in range(4)
                ],
                axis=1,
            )

        scaled_rows = [scaled(a) for a in range(4)]
        whole = jnp.concatenate(scaled_rows, axis=0)
        mixed = product(parts(whole[:, low]), pair(basis, low, ALL)) + product(
            parts(whole[:, high]), pair(basis, high, ALL)
        )
        upper, lower = parts(mixed[low]), parts(mixed[high])
        for k in range(2):
            rows = slice(k * half, (k + 1) * half)
            result[layer, rows] = product(pair(basis_t, rows, low), upper) + product(
                pair(basis_t, rows, high), lower
            )
            copies.append(
                pltpu.make_async_copy(
                    result.at[layer, rows], gradient.at[layer, rows], sems.at[4 + 2 * layer + k]
                )
            )
            copies[-1].start()
    for copy in copies:
        copy.wait()


def partner(index, phase):
    return index + 1 if index % 2 == phase else index - 1


def swap(value, axis, phase):
    count = lax.axis_size(axis)
    links = [(i, partner(i, phase)) for i in range(count)]
    return lax.ppermute(value, axis, [link for link in links if 0 <= link[1] < count])


def in_hbm(value):
    return pltpu.with_memory_space_constraint(value, pltpu.HBM)


def phases(axis):
    return [phase for phase in (1, 0) if lax.axis_size(axis) > 1 + phase]


def cost(units, tile):
    flops = int(units * 6 * tile**3)
    return pl.CostEstimate(flops=flops, bytes_accessed=tile * tile * 16, transcendentals=0)


def body(density, observed, stations, layer_index):
    layers, tile = density.shape[0], density.shape[1]
    xs, ys = phases("gx"), phases("gy")
    groups = 3 * (tile // 2)
    consts = [jnp.asarray(table) for table in tables(tile)]
    basis, sides = consts[:4], consts[4:]
    vmem = pl.BlockSpec(memory_space=pltpu.VMEM)
    hbm = pl.BlockSpec(memory_space=pltpu.HBM)

    def array(*shape):
        return jax.ShapeDtypeStruct(shape, F32)

    def cols_of(phase):
        upper = (lax.axis_index("gy") & 1) == phase
        return jnp.where(upper, density[..., tile - RADIUS :], density[..., :RADIUS])

    def rows_of(phase):
        upper = (lax.axis_index("gx") & 1) == phase
        both = jnp.stack([observed, stations.astype(F32)])
        return jnp.where(upper, both[:, tile - RADIUS :], both[:, :RADIUS])

    density_halos = [swap(cols_of(phase), "gy", phase) for phase in ys]
    strips = [swap(rows_of(phase), "gx", phase) for phase in xs]
    spectra = pl.pallas_call(
        functools.partial(spectrum_kernel, tile, layers),
        out_shape=array(layers, groups, groups),
        in_specs=[hbm] * 5,
        out_specs=vmem,
        scratch_shapes=[pltpu.VMEM(table.shape, BF16) for table in sides]
        + [pltpu.SMEM((layers,), jnp.int32), pltpu.SemaphoreType.DMA((5,))],
        compiler_params=PARAMS,
        cost_estimate=cost(8, tile),
        name="spectrum",
    )(*[in_hbm(value) for value in (layer_index, *sides)])
    early = int(len(xs) == 1 and 1 in ys)
    operands = [density, spectra, observed, stations, *density_halos, *basis]
    out = pl.pallas_call(
        functools.partial(forward_kernel, xs, ys, early, tile, layers),
        out_shape=[array(tile, tile)] * 2
        + [array(2 * RADIUS, RADIUS)] * (2 * len(xs))
        + [array(tile - RADIUS, RADIUS)] * early,
        in_specs=[vmem] * len(operands),
        out_specs=[vmem] * (2 + 2 * len(xs) + early),
        scratch_shapes=[pltpu.VMEM((layers * tile, tile), F32), pltpu.VMEM((2 * tile, 2 * tile), F32)],
        compiler_params=PARAMS,
        cost_estimate=cost(18, tile),
        name="forward",
    )(*operands)
    own, spill, sends, firsts = out[0], out[1], out[2 : 2 + 2 * len(xs)], out[2 + 2 * len(xs) :]
    sums = {other: [] for other in (1, 0)}
    for value, (phase, other) in zip(sends, itertools.product(xs, (1, 0))):
        sums[other].append(swap(value, "gx", phase))
    firsts = [swap(value, "gy", 1) for value in firsts]
    halves, received = [], []
    for other in (1, 0):
        operands = [own, spill, observed, stations, *sums[other], *strips]
        there = int(other in ys)
        tall = RADIUS * len(xs) + (RADIUS if early and other else tile)
        out = pl.pallas_call(
            functools.partial(side_kernel, xs, early, other, tile),
            out_shape=[array(tile, RADIUS)] * 3 + [array(tall, RADIUS)] * there,
            in_specs=[vmem] * len(operands),
            out_specs=[vmem] * (3 + there),
            compiler_params=PARAMS,
            cost_estimate=cost(1, tile),
        )(*operands)
        halves += out[:3]
        received += [swap(value, "gy", other) for value in out[3:]]
    operands = [spectra, *halves, *firsts, *received, *basis]
    return pl.pallas_call(
        functools.partial(adjoint_kernel, xs, ys, early, tile, layers),
        out_shape=[array(tile, tile), array(tile, tile), array(layers, tile, tile)],
        in_specs=[vmem] * len(operands),
        out_specs=[hbm] * 3,
        scratch_shapes=[pltpu.VMEM((tile, tile), F32)] * 4
        + [
            pltpu.VMEM((2 * tile, 2 * tile), F32),
            pltpu.VMEM((layers, tile, tile), F32),
            pltpu.SemaphoreType.DMA((4 + 2 * layers,)),
        ],
        compiler_params=PARAMS,
        cost_estimate=cost(20, tile),
        name="adjoint",
    )(*operands)


def solution(mesh):
    in_specs = (P(None, "gx", "gy"), P("gx", "gy"), P("gx", "gy"), P())
    out_specs = (P("gx", "gy"), P("gx", "gy"), P(None, "gx", "gy"))
    return jax.shard_map(body, mesh=mesh, in_specs=in_specs, out_specs=out_specs, check_vma=False)
```

```python
import functools
import itertools
import math

import jax
import jax.numpy as jnp
import ml_dtypes
import numpy as np
from jax import lax
from jax.experimental import pallas as pl
from jax.experimental.pallas import tpu as pltpu
from jax.sharding import PartitionSpec as P


RADIUS = 128
LAYERS_ALL = 512

F32 = jnp.float32
BF16 = jnp.bfloat16
PARAMS = pltpu.CompilerParams(vmem_limit_bytes=24 * 2**20)


def halves(table):
    table = table.astype(np.float32)
    high = table.astype(ml_dtypes.bfloat16)
    low = (table - high.astype(np.float32)).astype(ml_dtypes.bfloat16)
    return [high, low]


@functools.lru_cache(maxsize=None)
def tables(tile):
    length = 2 * tile
    half = tile // 2
    ticks = np.arange(tile)
    even = 2 * np.arange(half)
    odd = even + 1

    def angles(freqs):
        return (freqs[:, None] * ticks[None, :] % length) * (2.0 * math.pi / length)

    middle = even.copy()
    middle[0] = tile
    even_sin = np.sin(angles(even))
    even_sin[0] = np.cos(angles(middle))[0]
    basis = np.concatenate([np.cos(angles(even)), even_sin, np.cos(angles(odd)), np.sin(angles(odd))])
    fold = np.where(ticks == 0, 1.0, 2.0) * (ticks <= RADIUS)
    freqs = np.concatenate([even, middle, odd])
    weights = np.where((freqs == 0) | (freqs == tile), 1.0, 2.0) / length
    sides = np.cos(angles(freqs)) * fold[None, :] * weights[:, None]
    return halves(basis) + halves(basis.T) + halves(sides) + halves(sides.T)


def parts(value):
    high = value.astype(BF16)
    return high, (value - high.astype(F32)).astype(BF16)


def product(left, right):
    def dot(a, b):
        return jnp.dot(a, b, preferred_element_type=F32)

    return dot(left[0], right[0]) + (dot(left[0], right[1]) + dot(left[1], right[0]))


def pair(refs, *index):
    return refs[0][index], refs[1][index]


def side(axis, phase):
    return jnp.where((lax.axis_index(axis) & 1) == phase, 0, RADIUS)


def halo(axis, phase):
    return pl.ds(pl.multiple_of(side(axis, phase), RADIUS), RADIUS)


def edge(axis, phase):
    return pl.ds(pl.multiple_of(RADIUS - side(axis, phase), RADIUS), RADIUS)


def group(block, half):
    return slice(min(block, 2) * half, (min(block, 2) + 1) * half)


ALL = slice(None)


def spectrum_kernel(tile, layers, index_source, *refs):
    sources, spectra, held, index, sems = refs[:4], refs[4], refs[5:9], refs[9], refs[10]
    copies = [pltpu.make_async_copy(sources[k], held[k], sems.at[k]) for k in range(4)]
    copies.append(pltpu.make_async_copy(index_source, index, sems.at[4]))
    for copy in reversed(copies):
        copy.start()
    span = RADIUS + 8
    rows = lax.broadcasted_iota(jnp.int32, (span, tile), 0)
    cols = lax.broadcasted_iota(jnp.int32, (span, tile), 1)
    offsets = (rows * rows + cols * cols).astype(F32)
    copies[4].wait()
    values = []
    for layer in range(layers):
        depth = RADIUS * (0.375 + index[layer].astype(F32) / LAYERS_ALL)
        square = offsets + depth * depth
        values.append(depth * depth / (square * jnp.sqrt(square)))
    copies[2].wait()
    copies[3].wait()
    first = product(parts(jnp.concatenate(values, axis=0)), pair(held[2:], ALL, ALL))
    copies[0].wait()
    copies[1].wait()
    rest = jnp.zeros((tile - span, first.shape[1]), F32)
    for layer in range(layers):
        own = jnp.concatenate([first[layer * span : (layer + 1) * span], rest], axis=0)
        spectra[layer] = product(pair(held[:2], ALL, ALL), parts(own))


def forward_kernel(xs, ys, early, tile, layers, density, spectra, observed, stations, *refs):
    received, refs = refs[: len(ys)], refs[len(ys) :]
    basis, basis_t, (own, spill), refs = refs[:2], refs[2:4], refs[4:6], refs[6:]
    sends, firsts, (wrapped, total) = refs[: 2 * len(xs)], refs[2 * len(xs) : -2], refs[-2:]
    half = tile // 2
    low, high = slice(0, tile), slice(tile, 2 * tile)
    if len(ys) < 2:
        wrapped[...] = jnp.zeros_like(wrapped)
    for ref, phase in zip(received, ys):
        for layer in range(layers):
            wrapped[layer * tile : (layer + 1) * tile, halo("gy", phase)] = ref[layer]
    field = jnp.concatenate([density[layer] for layer in range(layers)], axis=0)
    behind = wrapped[...]
    even = product(parts(field + behind), pair(basis_t, ALL, low))
    odd = product(parts(field - behind), pair(basis_t, ALL, high))
    for layer in range(layers):
        rows = slice(layer * tile, (layer + 1) * tile)
        both = jnp.concatenate([even[rows], odd[rows]], axis=1)
        value = product(pair(basis, ALL, ALL), parts(both))
        for a in range(4):
            for b in range(4):
                place = slice(a * half, (a + 1) * half), slice(b * half, (b + 1) * half)
                term = spectra[layer, group(a, half), group(b, half)] * value[place]
                total[place] = term if layer == 0 else total[place] + term
    mixed = product(parts(total[:, low]), pair(basis, low, ALL)) + product(
        parts(total[:, high]), pair(basis, high, ALL)
    )
    even = product(pair(basis_t, ALL, low), parts(mixed[low]))
    odd = product(pair(basis_t, ALL, high), parts(mixed[high]))
    own[...] = even + odd
    spill[...] = even - odd
    for k, (phase, other) in enumerate(itertools.product(xs, (1, 0))):
        sends[k][:RADIUS] = spill[halo("gx", phase), edge("gy", other)]
        sends[k][RADIUS:] = own[edge("gx", phase), edge("gy", other)]
    if early:
        place = halo("gx", xs[0]), edge("gy", 1)
        firsts[0][...] = stations[place].astype(F32) * (own[place] - observed[place])


def side_kernel(xs, early, other, tile, own, spill, observed, stations, *refs):
    count = len(xs)
    received, strips, refs = refs[:count], refs[count : 2 * count], refs[2 * count :]
    (predicted, residual, behind), sends = refs[:3], refs[3:]
    cols = edge("gy", other)
    predicted[...] = own[:, cols]
    if count < 2:
        behind[...] = jnp.zeros_like(behind)
    for ref, strip, phase in zip(received, strips, xs):
        predicted[edge("gx", phase)] += ref[:RADIUS]
        rows = halo("gx", phase)
        behind[rows] = strip[1, :, cols] * (spill[rows, cols] + ref[RADIUS:] - strip[0, :, cols])
    residual[...] = stations[:, cols].astype(F32) * (predicted[...] - observed[:, cols])
    for ref in sends:
        if early and other:
            ref[:RADIUS] = residual[edge("gx", xs[0])]
        else:
            ref[:tile] = residual[...]
        for k, phase in enumerate(xs):
            start = ref.shape[0] + (k - count) * RADIUS
            ref[start : start + RADIUS] = behind[halo("gx", phase)]


def scaled(spectra, layer, value, half):
    rows = []
    for a in range(4):
        blocks = [
            spectra[layer, group(a, half), group(b, half)]
            * value[a * half : (a + 1) * half, b * half : (b + 1) * half]
            for b in range(4)
        ]
        rows.append(jnp.concatenate(blocks, axis=1))
    return jnp.concatenate(rows, axis=0)


def wide_product(left, right):
    width = right[0].shape[1]
    both = jnp.dot(left[0], jnp.concatenate(right, axis=1), preferred_element_type=F32)
    return both[:, :width] + (both[:, width:] + jnp.dot(left[1], right[0], preferred_element_type=F32))


def gradient_half(spectra, value, basis, basis_t, other, tile, layers):
    low, high = slice(0, tile), slice(tile, 2 * tile)
    table = pair(basis, ALL, edge("gy", other))
    mixed = [wide_product(parts(scaled(spectra, layer, value, tile // 2)), table) for layer in range(layers)]
    mixed = jnp.concatenate(mixed, axis=1)
    return product(pair(basis_t, ALL, low), parts(mixed[low])) + product(
        pair(basis_t, ALL, high), parts(mixed[high])
    )


def far_kernel(xs, paired, tile, layers, spectra, *refs):
    halves, refs = (refs[:3], refs[3:6]), refs[6:]
    strips, basis, basis_t = refs[: len(paired)], refs[len(paired) :][:2], refs[len(paired) :][2:4]
    refs = refs[len(paired) + 4 :]
    predicted_out, residual_out, field, result = refs[:4]
    residual, behind, across, corner, sems = refs[4:]
    low, high = slice(0, tile), slice(tile, 2 * tile)
    copies = []
    for k, other in enumerate((1, 0)):
        cols = edge("gy", other)
        copies.append(pltpu.make_async_copy(halves[k][0], predicted_out.at[:, cols], sems.at[2 * k]))
        copies.append(pltpu.make_async_copy(halves[k][1], residual_out.at[:, cols], sems.at[2 * k + 1]))
    for copy in copies:
        copy.start()
    for k, other in enumerate((1, 0)):
        residual[:, edge("gy", other)] = halves[k][1][...]
        behind[:, edge("gy", other)] = halves[k][2][...]
    across[...] = jnp.zeros_like(across)
    corner[...] = jnp.zeros_like(corner)
    for ref, phase in zip(strips, paired):
        cols = halo("gy", phase)
        across[:, cols] = ref[:tile]
        for k, other in enumerate(xs):
            start = tile + k * RADIUS
            corner[halo("gx", other), cols] = ref[start : start + RADIUS]
    up_even, up_odd = residual[...] + across[...], residual[...] - across[...]
    down_even, down_odd = behind[...] + corner[...], behind[...] - corner[...]
    even = jnp.concatenate([up_even + down_even, up_even - down_even], axis=0)
    odd = jnp.concatenate([up_odd + down_odd, up_odd - down_odd], axis=0)
    even = product(parts(even), pair(basis_t, ALL, low))
    odd = product(parts(odd), pair(basis_t, ALL, high))
    for rows in (low, high):
        both = jnp.concatenate([even[rows], odd[rows]], axis=1)
        field[rows] = product(pair(basis, rows, ALL), parts(both))
    result[...] = gradient_half(spectra, field, basis, basis_t, 0, tile, layers)
    for copy in copies:
        copy.wait()


def adjoint_kernel(xs, crossing, early, tile, layers, spectra, field, far, *refs):
    firsts, refs = refs[:early], refs[early:]
    strips, basis, basis_t = refs[: len(crossing)], refs[len(crossing) :][:2], refs[len(crossing) :][2:4]
    gradient, across, corner, held, result, sems = refs[len(crossing) + 4 :]
    low, high = slice(0, tile), slice(tile, 2 * tile)
    copies = []

    def put(source, first, other):
        for layer in range(layers):
            here = source.at[:, layer * RADIUS : (layer + 1) * RADIUS]
            there = gradient.at[layer, :, edge("gy", other)]
            copies.append(pltpu.make_async_copy(here, there, sems.at[first + layer]))
            copies[-1].start()

    put(far, 0, 0)
    for ref, phase in zip(strips, crossing):
        if len(xs) < 2:
            corner[...] = jnp.zeros_like(corner)
        if early:
            across[halo("gx", xs[0])] = firsts[0][...]
            across[edge("gx", xs[0])] = ref[:RADIUS]
        else:
            across[...] = ref[:tile]
        for k, other in enumerate(xs):
            start = ref.shape[0] + (k - len(xs)) * RADIUS
            corner[halo("gx", other)] = ref[start : start + RADIUS]
        up = wide_product(pair(basis, low, ALL), parts(across[...] + corner[...]))
        down = wide_product(pair(basis, high, ALL), parts(across[...] - corner[...]))
        both = jnp.concatenate(parts(jnp.concatenate([up, down], axis=0)), axis=1)
        ticks = halo("gy", phase)
        upper, lower = (jnp.concatenate([table[ticks, :]] * 2, axis=0) for table in basis_t)
        value = jnp.dot(both, upper, preferred_element_type=F32) + jnp.dot(both, lower, preferred_element_type=F32)
        held[:, low] = field[:, low] + value[:, low]
        held[:, high] = field[:, high] - value[:, high]
    result[...] = gradient_half(spectra, held if crossing else field, basis, basis_t, 1, tile, layers)
    put(result, layers, 1)
    for copy in copies:
        copy.wait()


def partner(index, phase):
    return index + 1 if index % 2 == phase else index - 1


def swap(value, axis, phase):
    count = lax.axis_size(axis)
    links = [(i, partner(i, phase)) for i in range(count)]
    return lax.ppermute(value, axis, [link for link in links if 0 <= link[1] < count])


def in_hbm(value):
    return pltpu.with_memory_space_constraint(value, pltpu.HBM)


def phases(axis):
    return [phase for phase in (1, 0) if lax.axis_size(axis) > 1 + phase]


def cost(units, tile):
    flops = int(units * 6 * tile**3)
    return pl.CostEstimate(flops=flops, bytes_accessed=tile * tile * 16, transcendentals=0)


def body(density, observed, stations, layer_index):
    layers, tile = density.shape[0], density.shape[1]
    xs, ys = phases("gx"), phases("gy")
    groups = 3 * (tile // 2)
    consts = [jnp.asarray(table) for table in tables(tile)]
    basis, sides = consts[:4], consts[4:]
    vmem = pl.BlockSpec(memory_space=pltpu.VMEM)
    hbm = pl.BlockSpec(memory_space=pltpu.HBM)

    def array(*shape):
        return jax.ShapeDtypeStruct(shape, F32)

    def cols_of(phase):
        upper = (lax.axis_index("gy") & 1) == phase
        return jnp.where(upper, density[..., tile - RADIUS :], density[..., :RADIUS])

    def rows_of(phase):
        upper = (lax.axis_index("gx") & 1) == phase
        both = jnp.stack([observed, stations.astype(F32)])
        return jnp.where(upper, both[:, tile - RADIUS :], both[:, :RADIUS])

    density_halos = [swap(cols_of(phase), "gy", phase) for phase in ys]
    strips = [swap(rows_of(phase), "gx", phase) for phase in xs]
    spectra = pl.pallas_call(
        functools.partial(spectrum_kernel, tile, layers),
        out_shape=array(layers, groups, groups),
        in_specs=[hbm] * 5,
        out_specs=vmem,
        scratch_shapes=[pltpu.VMEM(table.shape, BF16) for table in sides]
        + [pltpu.SMEM((layers,), jnp.int32), pltpu.SemaphoreType.DMA((5,))],
        compiler_params=PARAMS,
        cost_estimate=cost(8, tile),
        name="spectrum",
    )(*[in_hbm(value) for value in (layer_index, *sides)])
    early = int(len(xs) == 1 and 1 in ys)
    operands = [density, spectra, observed, stations, *density_halos, *basis]
    out = pl.pallas_call(
        functools.partial(forward_kernel, xs, ys, early, tile, layers),
        out_shape=[array(tile, tile)] * 2
        + [array(2 * RADIUS, RADIUS)] * (2 * len(xs))
        + [array(tile - RADIUS, RADIUS)] * early,
        in_specs=[vmem] * len(operands),
        out_specs=[vmem] * (2 + 2 * len(xs) + early),
        scratch_shapes=[pltpu.VMEM((layers * tile, tile), F32), pltpu.VMEM((2 * tile, 2 * tile), F32)],
        compiler_params=PARAMS,
        cost_estimate=cost(18, tile),
        name="forward",
    )(*operands)
    own, spill, sends, firsts = out[0], out[1], out[2 : 2 + 2 * len(xs)], out[2 + 2 * len(xs) :]
    sums = {other: [] for other in (1, 0)}
    for value, (phase, other) in zip(sends, itertools.product(xs, (1, 0))):
        sums[other].append(swap(value, "gx", phase))
    firsts = [swap(value, "gy", 1) for value in firsts]
    halves, received = [], []
    for other in (1, 0):
        operands = [own, spill, observed, stations, *sums[other], *strips]
        there = int(other in ys)
        tall = RADIUS * len(xs) + (RADIUS if early and other else tile)
        out = pl.pallas_call(
            functools.partial(side_kernel, xs, early, other, tile),
            out_shape=[array(tile, RADIUS)] * 3 + [array(tall, RADIUS)] * there,
            in_specs=[vmem] * len(operands),
            out_specs=[vmem] * (3 + there),
            compiler_params=PARAMS,
            cost_estimate=cost(1, tile),
        )(*operands)
        halves += out[:3]
        received += [swap(value, "gy", other) for value in out[3:]]
    crossing = [phase for phase in ys if phase]
    paired = [phase for phase in ys if not phase]
    operands = [spectra, *halves, *received[len(crossing) :], *basis]
    predicted, residual, field, far = pl.pallas_call(
        functools.partial(far_kernel, xs, paired, tile, layers),
        out_shape=[array(tile, tile)] * 2 + [array(2 * tile, 2 * tile), array(tile, layers * RADIUS)],
        in_specs=[vmem] * len(operands),
        out_specs=[hbm] * 2 + [vmem] * 2,
        scratch_shapes=[pltpu.VMEM((tile, tile), F32)] * 4 + [pltpu.SemaphoreType.DMA((4,))],
        compiler_params=PARAMS,
        cost_estimate=cost(16, tile),
        name="far",
    )(*operands)
    operands = [spectra, field, far, *firsts, *received[: len(crossing)], *basis]
    gradient = pl.pallas_call(
        functools.partial(adjoint_kernel, xs, crossing, early, tile, layers),
        out_shape=array(layers, tile, tile),
        in_specs=[vmem] * len(operands),
        out_specs=hbm,
        scratch_shapes=[pltpu.VMEM((tile, RADIUS), F32)] * 2
        + [
            pltpu.VMEM((2 * tile, 2 * tile), F32),
            pltpu.VMEM((tile, layers * RADIUS), F32),
            pltpu.SemaphoreType.DMA((2 * layers,)),
        ],
        compiler_params=PARAMS,
        cost_estimate=cost(12, tile),
        name="adjoint",
    )(*operands)
    return predicted, residual, gradient


def solution(mesh):
    in_specs = (P(None, "gx", "gy"), P("gx", "gy"), P("gx", "gy"), P())
    out_specs = (P("gx", "gy"), P("gx", "gy"), P(None, "gx", "gy"))
    return jax.shard_map(body, mesh=mesh, in_specs=in_specs, out_specs=out_specs, check_vma=False)
```

```python
import functools
import itertools
import math

import jax
import jax.numpy as jnp
import ml_dtypes
import numpy as np
from jax import lax
from jax.experimental import pallas as pl
from jax.experimental.pallas import tpu as pltpu
from jax.sharding import PartitionSpec as P


RADIUS = 128
LAYERS_ALL = 512

F32 = jnp.float32
BF16 = jnp.bfloat16
PARAMS = pltpu.CompilerParams(vmem_limit_bytes=24 * 2**20)


def halves(table):
    table = table.astype(np.float32)
    high = table.astype(ml_dtypes.bfloat16)
    low = (table - high.astype(np.float32)).astype(ml_dtypes.bfloat16)
    return [high, low]


@functools.lru_cache(maxsize=None)
def tables(tile):
    length = 2 * tile
    half = tile // 2
    ticks = np.arange(tile)
    even = 2 * np.arange(half)
    odd = even + 1

    def angles(freqs):
        return (freqs[:, None] * ticks[None, :] % length) * (2.0 * math.pi / length)

    middle = even.copy()
    middle[0] = tile
    even_sin = np.sin(angles(even))
    even_sin[0] = np.cos(angles(middle))[0]
    basis = np.concatenate([np.cos(angles(even)), even_sin, np.cos(angles(odd)), np.sin(angles(odd))])
    fold = np.where(ticks == 0, 1.0, 2.0) * (ticks <= RADIUS)
    freqs = np.concatenate([even, middle, odd])
    weights = np.where((freqs == 0) | (freqs == tile), 1.0, 2.0) / length
    sides = np.cos(angles(freqs)) * fold[None, :] * weights[:, None]
    return halves(basis) + halves(basis.T) + halves(sides) + halves(sides.T)


def parts(value):
    high = value.astype(BF16)
    return high, (value - high.astype(F32)).astype(BF16)


def product(left, right):
    def dot(a, b):
        return jnp.dot(a, b, preferred_element_type=F32)

    return dot(left[0], right[0]) + (dot(left[0], right[1]) + dot(left[1], right[0]))


def pair(refs, *index):
    return refs[0][index], refs[1][index]


def side(axis, phase):
    return jnp.where((lax.axis_index(axis) & 1) == phase, 0, RADIUS)


def halo(axis, phase):
    return pl.ds(pl.multiple_of(side(axis, phase), RADIUS), RADIUS)


def edge(axis, phase):
    return pl.ds(pl.multiple_of(RADIUS - side(axis, phase), RADIUS), RADIUS)


def group(block, half):
    return slice(min(block, 2) * half, (min(block, 2) + 1) * half)


ALL = slice(None)


def spectrum_kernel(tile, layers, index_source, *refs):
    sources, spectra, held, index, sems = refs[:4], refs[4], refs[5:9], refs[9], refs[10]
    copies = [pltpu.make_async_copy(sources[k], held[k], sems.at[k]) for k in range(4)]
    copies.append(pltpu.make_async_copy(index_source, index, sems.at[4]))
    for copy in reversed(copies):
        copy.start()
    span = RADIUS + 8
    rows = lax.broadcasted_iota(jnp.int32, (span, tile), 0)
    cols = lax.broadcasted_iota(jnp.int32, (span, tile), 1)
    offsets = (rows * rows + cols * cols).astype(F32)
    copies[4].wait()
    values = []
    for layer in range(layers):
        depth = RADIUS * (0.375 + index[layer].astype(F32) / LAYERS_ALL)
        square = offsets + depth * depth
        values.append(depth * depth / (square * jnp.sqrt(square)))
    copies[2].wait()
    copies[3].wait()
    first = product(parts(jnp.concatenate(values, axis=0)), pair(held[2:], ALL, ALL))
    copies[0].wait()
    copies[1].wait()
    rest = jnp.zeros((tile - span, first.shape[1]), F32)
    for layer in range(layers):
        own = jnp.concatenate([first[layer * span : (layer + 1) * span], rest], axis=0)
        spectra[layer] = product(pair(held[:2], ALL, ALL), parts(own))


def forward_kernel(xs, ys, early, tile, layers, density, spectra, observed, stations, *refs):
    received, refs = refs[: len(ys)], refs[len(ys) :]
    basis, basis_t, (own, spill), refs = refs[:2], refs[2:4], refs[4:6], refs[6:]
    sends, firsts, (wrapped, total) = refs[: 2 * len(xs)], refs[2 * len(xs) : -2], refs[-2:]
    half = tile // 2
    low, high = slice(0, tile), slice(tile, 2 * tile)
    if len(ys) < 2:
        wrapped[...] = jnp.zeros_like(wrapped)
    for ref, phase in zip(received, ys):
        for layer in range(layers):
            wrapped[layer * tile : (layer + 1) * tile, halo("gy", phase)] = ref[layer]
    field = jnp.concatenate([density[layer] for layer in range(layers)], axis=0)
    behind = wrapped[...]
    even = product(parts(field + behind), pair(basis_t, ALL, low))
    odd = product(parts(field - behind), pair(basis_t, ALL, high))
    for layer in range(layers):
        rows = slice(layer * tile, (layer + 1) * tile)
        both = jnp.concatenate([even[rows], odd[rows]], axis=1)
        value = product(pair(basis, ALL, ALL), parts(both))
        for a in range(4):
            for b in range(4):
                place = slice(a * half, (a + 1) * half), slice(b * half, (b + 1) * half)
                term = spectra[layer, group(a, half), group(b, half)] * value[place]
                total[place] = term if layer == 0 else total[place] + term
    mixed = product(parts(total[:, low]), pair(basis, low, ALL)) + product(
        parts(total[:, high]), pair(basis, high, ALL)
    )
    even = product(pair(basis_t, ALL, low), parts(mixed[low]))
    odd = product(pair(basis_t, ALL, high), parts(mixed[high]))
    own[...] = even + odd
    spill[...] = even - odd
    for k, (phase, other) in enumerate(itertools.product(xs, (1, 0))):
        sends[k][:RADIUS] = spill[halo("gx", phase), edge("gy", other)]
        sends[k][RADIUS:] = own[edge("gx", phase), edge("gy", other)]
    if early:
        place = halo("gx", xs[0]), edge("gy", 1)
        firsts[0][...] = stations[place].astype(F32) * (own[place] - observed[place])


def side_kernel(xs, early, other, tile, own, spill, observed, stations, *refs):
    count = len(xs)
    received, strips, refs = refs[:count], refs[count : 2 * count], refs[2 * count :]
    (predicted, residual, behind), sends = refs[:3], refs[3:]
    cols = edge("gy", other)
    predicted[...] = own[:, cols]
    if count < 2:
        behind[...] = jnp.zeros_like(behind)
    for ref, strip, phase in zip(received, strips, xs):
        predicted[edge("gx", phase)] += ref[:RADIUS]
        rows = halo("gx", phase)
        behind[rows] = strip[1, :, cols] * (spill[rows, cols] + ref[RADIUS:] - strip[0, :, cols])
    residual[...] = stations[:, cols].astype(F32) * (predicted[...] - observed[:, cols])
    for ref in sends:
        if early and other:
            ref[:RADIUS] = residual[edge("gx", xs[0])]
        else:
            ref[:tile] = residual[...]
        for k, phase in enumerate(xs):
            start = ref.shape[0] + (k - count) * RADIUS
            ref[start : start + RADIUS] = behind[halo("gx", phase)]


def scaled(spectra, layer, value, half):
    rows = []
    for a in range(4):
        blocks = [
            spectra[layer, group(a, half), group(b, half)]
            * value[a * half : (a + 1) * half, b * half : (b + 1) * half]
            for b in range(4)
        ]
        rows.append(jnp.concatenate(blocks, axis=1))
    return jnp.concatenate(rows, axis=0)


def wide_product(left, right):
    width = right[0].shape[1]
    both = jnp.dot(left[0], jnp.concatenate(right, axis=1), preferred_element_type=F32)
    return both[:, :width] + (both[:, width:] + jnp.dot(left[1], right[0], preferred_element_type=F32))


def gradient_half(spectra, value, basis, basis_t, other, tile, layers):
    low, high = slice(0, tile), slice(tile, 2 * tile)
    table = pair(basis, ALL, edge("gy", other))
    mixed = [wide_product(parts(scaled(spectra, layer, value, tile // 2)), table) for layer in range(layers)]
    mixed = jnp.concatenate(mixed, axis=1)
    return product(pair(basis_t, ALL, low), parts(mixed[low])) + product(
        pair(basis_t, ALL, high), parts(mixed[high])
    )


def own_kernel(tile, *refs):
    halves, basis = (refs[:3], refs[3:6]), refs[6:8]
    predicted_out, residual_out, rows_done, residual, behind, sems = refs[8:]
    low, high = slice(0, tile), slice(tile, 2 * tile)
    copies = []
    for k, other in enumerate((1, 0)):
        cols = edge("gy", other)
        copies.append(pltpu.make_async_copy(halves[k][0], predicted_out.at[:, cols], sems.at[2 * k]))
        copies.append(pltpu.make_async_copy(halves[k][1], residual_out.at[:, cols], sems.at[2 * k + 1]))
    for copy in copies:
        copy.start()
    for k, other in enumerate((1, 0)):
        residual[:, edge("gy", other)] = halves[k][1][...]
        behind[:, edge("gy", other)] = halves[k][2][...]
    rows_done[low] = product(pair(basis, low, ALL), parts(residual[...] + behind[...]))
    rows_done[high] = product(pair(basis, high, ALL), parts(residual[...] - behind[...]))
    for copy in copies:
        copy.wait()


def strip_rows(top, bottom, basis, tile):
    up = wide_product(pair(basis, slice(0, tile), ALL), parts(top + bottom))
    down = wide_product(pair(basis, slice(tile, 2 * tile), ALL), parts(top - bottom))
    return jnp.concatenate([up, down], axis=0)


def far_kernel(xs, paired, tile, layers, spectra, rows_done, *refs):
    strips, refs = refs[: len(paired)], refs[len(paired) :]
    basis, basis_t, (field, result, corner, wrapped) = refs[:2], refs[2:4], refs[4:]
    low, high = slice(0, tile), slice(tile, 2 * tile)
    wrapped[...] = jnp.zeros_like(wrapped)
    for ref, phase in zip(strips, paired):
        if len(xs) < 2:
            corner[...] = jnp.zeros_like(corner)
        for k, other in enumerate(xs):
            start = tile + k * RADIUS
            corner[halo("gx", other)] = ref[start : start + RADIUS]
        wrapped[:, halo("gy", phase)] = strip_rows(ref[:tile], corner[...], basis, tile)
    field[:, low] = product(parts(rows_done[...] + wrapped[...]), pair(basis_t, ALL, low))
    field[:, high] = product(parts(rows_done[...] - wrapped[...]), pair(basis_t, ALL, high))
    result[...] = gradient_half(spectra, field, basis, basis_t, 0, tile, layers)


def adjoint_kernel(xs, crossing, early, tile, layers, spectra, field, far, *refs):
    firsts, refs = refs[:early], refs[early:]
    strips, basis, basis_t = refs[: len(crossing)], refs[len(crossing) :][:2], refs[len(crossing) :][2:4]
    gradient, across, corner, held, result, sems = refs[len(crossing) + 4 :]
    low, high = slice(0, tile), slice(tile, 2 * tile)
    copies = []

    def put(source, first, other):
        for layer in range(layers):
            here = source.at[:, layer * RADIUS : (layer + 1) * RADIUS]
            there = gradient.at[layer, :, edge("gy", other)]
            copies.append(pltpu.make_async_copy(here, there, sems.at[first + layer]))
            copies[-1].start()

    put(far, 0, 0)
    for ref, phase in zip(strips, crossing):
        if len(xs) < 2:
            corner[...] = jnp.zeros_like(corner)
        if early:
            across[halo("gx", xs[0])] = firsts[0][...]
            across[edge("gx", xs[0])] = ref[:RADIUS]
        else:
            across[...] = ref[:tile]
        for k, other in enumerate(xs):
            start = ref.shape[0] + (k - len(xs)) * RADIUS
            corner[halo("gx", other)] = ref[start : start + RADIUS]
        both = jnp.concatenate(parts(strip_rows(across[...], corner[...], basis, tile)), axis=1)
        ticks = halo("gy", phase)
        upper, lower = (jnp.concatenate([table[ticks, :]] * 2, axis=0) for table in basis_t)
        value = jnp.dot(both, upper, preferred_element_type=F32) + jnp.dot(both, lower, preferred_element_type=F32)
        held[:, low] = field[:, low] + value[:, low]
        held[:, high] = field[:, high] - value[:, high]
    result[...] = gradient_half(spectra, held if crossing else field, basis, basis_t, 1, tile, layers)
    put(result, layers, 1)
    for copy in copies:
        copy.wait()


def partner(index, phase):
    return index + 1 if index % 2 == phase else index - 1


def swap(value, axis, phase):
    count = lax.axis_size(axis)
    links = [(i, partner(i, phase)) for i in range(count)]
    return lax.ppermute(value, axis, [link for link in links if 0 <= link[1] < count])


def in_hbm(value):
    return pltpu.with_memory_space_constraint(value, pltpu.HBM)


def phases(axis):
    return [phase for phase in (1, 0) if lax.axis_size(axis) > 1 + phase]


def cost(units, tile):
    flops = int(units * 6 * tile**3)
    return pl.CostEstimate(flops=flops, bytes_accessed=tile * tile * 16, transcendentals=0)


def body(density, observed, stations, layer_index):
    layers, tile = density.shape[0], density.shape[1]
    xs, ys = phases("gx"), phases("gy")
    groups = 3 * (tile // 2)
    consts = [jnp.asarray(table) for table in tables(tile)]
    basis, sides = consts[:4], consts[4:]
    vmem = pl.BlockSpec(memory_space=pltpu.VMEM)
    hbm = pl.BlockSpec(memory_space=pltpu.HBM)

    def array(*shape):
        return jax.ShapeDtypeStruct(shape, F32)

    def cols_of(phase):
        upper = (lax.axis_index("gy") & 1) == phase
        return jnp.where(upper, density[..., tile - RADIUS :], density[..., :RADIUS])

    def rows_of(phase):
        upper = (lax.axis_index("gx") & 1) == phase
        both = jnp.stack([observed, stations.astype(F32)])
        return jnp.where(upper, both[:, tile - RADIUS :], both[:, :RADIUS])

    density_halos = [swap(cols_of(phase), "gy", phase) for phase in ys]
    strips = [swap(rows_of(phase), "gx", phase) for phase in xs]
    spectra = pl.pallas_call(
        functools.partial(spectrum_kernel, tile, layers),
        out_shape=array(layers, groups, groups),
        in_specs=[hbm] * 5,
        out_specs=vmem,
        scratch_shapes=[pltpu.VMEM(table.shape, BF16) for table in sides]
        + [pltpu.SMEM((layers,), jnp.int32), pltpu.SemaphoreType.DMA((5,))],
        compiler_params=PARAMS,
        cost_estimate=cost(8, tile),
        name="spectrum",
    )(*[in_hbm(value) for value in (layer_index, *sides)])
    early = int(len(xs) == 1 and 1 in ys)
    operands = [density, spectra, observed, stations, *density_halos, *basis]
    out = pl.pallas_call(
        functools.partial(forward_kernel, xs, ys, early, tile, layers),
        out_shape=[array(tile, tile)] * 2
        + [array(2 * RADIUS, RADIUS)] * (2 * len(xs))
        + [array(tile - RADIUS, RADIUS)] * early,
        in_specs=[vmem] * len(operands),
        out_specs=[vmem] * (2 + 2 * len(xs) + early),
        scratch_shapes=[pltpu.VMEM((layers * tile, tile), F32), pltpu.VMEM((2 * tile, 2 * tile), F32)],
        compiler_params=PARAMS,
        cost_estimate=cost(18, tile),
        name="forward",
    )(*operands)
    own, spill, sends, firsts = out[0], out[1], out[2 : 2 + 2 * len(xs)], out[2 + 2 * len(xs) :]
    sums = {other: [] for other in (1, 0)}
    for value, (phase, other) in zip(sends, itertools.product(xs, (1, 0))):
        sums[other].append(swap(value, "gx", phase))
    firsts = [swap(value, "gy", 1) for value in firsts]
    halves, received = [], []
    for other in (1, 0):
        operands = [own, spill, observed, stations, *sums[other], *strips]
        there = int(other in ys)
        tall = RADIUS * len(xs) + (RADIUS if early and other else tile)
        out = pl.pallas_call(
            functools.partial(side_kernel, xs, early, other, tile),
            out_shape=[array(tile, RADIUS)] * 3 + [array(tall, RADIUS)] * there,
            in_specs=[vmem] * len(operands),
            out_specs=[vmem] * (3 + there),
            compiler_params=PARAMS,
            cost_estimate=cost(1, tile),
        )(*operands)
        halves += out[:3]
        received += [swap(value, "gy", other) for value in out[3:]]
    crossing = [phase for phase in ys if phase]
    paired = [phase for phase in ys if not phase]
    operands = [*halves, *basis[:2]]
    predicted, residual, rows_done = pl.pallas_call(
        functools.partial(own_kernel, tile),
        out_shape=[array(tile, tile)] * 2 + [array(2 * tile, tile)],
        in_specs=[vmem] * len(operands),
        out_specs=[hbm] * 2 + [vmem],
        scratch_shapes=[pltpu.VMEM((tile, tile), F32)] * 2 + [pltpu.SemaphoreType.DMA((4,))],
        compiler_params=PARAMS,
        cost_estimate=cost(2, tile),
        name="own",
    )(*operands)
    operands = [spectra, rows_done, *received[len(crossing) :], *basis]
    field, far = pl.pallas_call(
        functools.partial(far_kernel, xs, paired, tile, layers),
        out_shape=[array(2 * tile, 2 * tile), array(tile, layers * RADIUS)],
        in_specs=[vmem] * len(operands),
        out_specs=[vmem] * 2,
        scratch_shapes=[pltpu.VMEM((tile, RADIUS), F32), pltpu.VMEM((2 * tile, tile), F32)],
        compiler_params=PARAMS,
        cost_estimate=cost(14, tile),
        name="far",
    )(*operands)
    operands = [spectra, field, far, *firsts, *received[: len(crossing)], *basis]
    gradient = pl.pallas_call(
        functools.partial(adjoint_kernel, xs, crossing, early, tile, layers),
        out_shape=array(layers, tile, tile),
        in_specs=[vmem] * len(operands),
        out_specs=hbm,
        scratch_shapes=[pltpu.VMEM((tile, RADIUS), F32)] * 2
        + [
            pltpu.VMEM((2 * tile, 2 * tile), F32),
            pltpu.VMEM((tile, layers * RADIUS), F32),
            pltpu.SemaphoreType.DMA((2 * layers,)),
        ],
        compiler_params=PARAMS,
        cost_estimate=cost(12, tile),
        name="adjoint",
    )(*operands)
    return predicted, residual, gradient


def solution(mesh):
    in_specs = (P(None, "gx", "gy"), P("gx", "gy"), P("gx", "gy"), P())
    out_specs = (P("gx", "gy"), P("gx", "gy"), P(None, "gx", "gy"))
    return jax.shard_map(body, mesh=mesh, in_specs=in_specs, out_specs=out_specs, check_vma=False)
```

```python
import functools
import math

import jax
import jax.numpy as jnp
import ml_dtypes
import numpy as np
from jax import lax
from jax.experimental import pallas as pl
from jax.experimental.pallas import tpu as pltpu
from jax.sharding import PartitionSpec as P


RADIUS = 128
LAYERS_ALL = 512

F32 = jnp.float32
BF16 = jnp.bfloat16
PARAMS = pltpu.CompilerParams(vmem_limit_bytes=24 * 2**20)


def halves(table):
    table = table.astype(np.float32)
    high = table.astype(ml_dtypes.bfloat16)
    low = (table - high.astype(np.float32)).astype(ml_dtypes.bfloat16)
    return [high, low]


@functools.lru_cache(maxsize=None)
def tables(tile):
    length = 2 * tile
    half = tile // 2
    ticks = np.arange(tile)
    even = 2 * np.arange(half)
    odd = even + 1

    def angles(freqs):
        return (freqs[:, None] * ticks[None, :] % length) * (2.0 * math.pi / length)

    middle = even.copy()
    middle[0] = tile
    even_sin = np.sin(angles(even))
    even_sin[0] = np.cos(angles(middle))[0]
    basis = np.concatenate([np.cos(angles(even)), even_sin, np.cos(angles(odd)), np.sin(angles(odd))])
    fold = np.where(ticks == 0, 1.0, 2.0) * (ticks <= RADIUS)
    freqs = np.concatenate([even, middle, odd])
    weights = np.where((freqs == 0) | (freqs == tile), 1.0, 2.0) / length
    sides = np.cos(angles(freqs)) * fold[None, :] * weights[:, None]
    return halves(basis) + halves(basis.T) + halves(sides) + halves(sides.T)


def parts(value):
    high = value.astype(BF16)
    return high, (value - high.astype(F32)).astype(BF16)


def product(left, right):
    def dot(a, b):
        return jnp.dot(a, b, preferred_element_type=F32)

    return dot(left[0], right[0]) + (dot(left[0], right[1]) + dot(left[1], right[0]))


def wide_product(left, right):
    width = right[0].shape[1]
    both = jnp.dot(left[0], jnp.concatenate(right, axis=1), preferred_element_type=F32)
    return both[:, :width] + (both[:, width:] + jnp.dot(left[1], right[0], preferred_element_type=F32))


def pair(refs, *index):
    return refs[0][index], refs[1][index]


def side(axis, phase):
    return jnp.where((lax.axis_index(axis) & 1) == phase, 0, RADIUS)


def halo(axis, phase):
    return pl.ds(pl.multiple_of(side(axis, phase), RADIUS), RADIUS)


def edge(axis, phase):
    return pl.ds(pl.multiple_of(RADIUS - side(axis, phase), RADIUS), RADIUS)


def group(block, half):
    return slice(min(block, 2) * half, (min(block, 2) + 1) * half)


ALL = slice(None)


def columns_half(total, basis, basis_t, other, tile):
    low, high = slice(0, tile), slice(tile, 2 * tile)
    mixed = wide_product(parts(total), pair(basis, ALL, edge("gy", other)))
    even = wide_product(pair(basis_t, ALL, low), parts(mixed[low]))
    odd = wide_product(pair(basis_t, ALL, high), parts(mixed[high]))
    return even + odd, even - odd


def send_half(xs, sends, own, spill):
    for ref, phase in zip(sends, xs):
        ref[:RADIUS] = spill[halo("gx", phase)]
        ref[RADIUS:] = own[edge("gx", phase)]


def summed(spectra, values, half, before=None):
    rows = []
    for a in range(4):
        blocks = []
        for b in range(4):
            place = slice(a * half, (a + 1) * half), slice(b * half, (b + 1) * half)
            block = None
            for layer, value in enumerate(values):
                term = spectra[layer, group(a, half), group(b, half)] * value[place]
                block = term if block is None else block + term
            if before is not None:
                block = before[place] + block if b < 2 else before[place] - block
            blocks.append(block)
        rows.append(jnp.concatenate(blocks, axis=1))
    return jnp.concatenate(rows, axis=0)


def prepare_kernel(xs, paired, tile, layers, index_source, *refs):
    sources, density, refs = refs[:4], refs[4], refs[5:]
    received, refs = refs[: len(paired)], refs[len(paired) :]
    basis, basis_t, (spectra, total, own, spill), refs = refs[:2], refs[2:4], refs[4:8], refs[8:]
    sends, held, (index, wrapped, fields, sems) = refs[: len(xs)], refs[len(xs) : len(xs) + 4], refs[len(xs) + 4 :]
    copies = [pltpu.make_async_copy(sources[k], held[k], sems.at[k]) for k in range(4)]
    copies.append(pltpu.make_async_copy(index_source, index, sems.at[4]))
    for copy in reversed(copies):
        copy.start()
    low, high = slice(0, tile), slice(tile, 2 * tile)
    wrapped[...] = jnp.zeros_like(wrapped)
    for ref, phase in zip(received, paired):
        for layer in range(layers):
            wrapped[layer * tile : (layer + 1) * tile, halo("gy", phase)] = ref[layer]
    field = jnp.concatenate([density[layer] for layer in range(layers)], axis=0)
    behind = wrapped[...]
    even = product(parts(field + behind), pair(basis_t, ALL, low))
    odd = product(parts(field - behind), pair(basis_t, ALL, high))
    for layer in range(layers):
        rows = slice(layer * tile, (layer + 1) * tile)
        both = jnp.concatenate([even[rows], odd[rows]], axis=1)
        fields[layer] = product(pair(basis, ALL, ALL), parts(both))
    span = RADIUS + 8
    rows = lax.broadcasted_iota(jnp.int32, (span, tile), 0)
    cols = lax.broadcasted_iota(jnp.int32, (span, tile), 1)
    offsets = (rows * rows + cols * cols).astype(F32)
    copies[4].wait()
    values = []
    for layer in range(layers):
        depth = RADIUS * (0.375 + index[layer].astype(F32) / LAYERS_ALL)
        square = offsets + depth * depth
        values.append(depth * depth / (square * jnp.sqrt(square)))
    copies[2].wait()
    copies[3].wait()
    first = product(parts(jnp.concatenate(values, axis=0)), pair(held[2:], ALL, ALL))
    copies[0].wait()
    copies[1].wait()
    rest = jnp.zeros((tile - span, first.shape[1]), F32)
    for layer in range(layers):
        whole = jnp.concatenate([first[layer * span : (layer + 1) * span], rest], axis=0)
        spectra[layer] = product(pair(held[:2], ALL, ALL), parts(whole))
    total[...] = summed(spectra, [fields.at[layer] for layer in range(layers)], tile // 2)
    own[...], spill[...] = columns_half(total[...], basis, basis_t, 0, tile)
    send_half(xs, sends, own, spill)


def forward_kernel(xs, crossing, early, tile, layers, spectra, before, observed, stations, *refs):
    received, refs = refs[: len(crossing)], refs[len(crossing) :]
    basis, basis_t, (own, spill), refs = refs[:2], refs[2:4], refs[4:6], refs[6:]
    sends, firsts = refs[: len(xs)], refs[len(xs) :]
    total = before[...]
    for ref, phase in zip(received, crossing):
        strips = jnp.concatenate([ref[layer] for layer in range(layers)], axis=1)
        rows_done = product(pair(basis, ALL, ALL), parts(strips))
        ticks = halo("gy", phase)
        upper, lower = (jnp.concatenate([table[ticks, :]] * 2, axis=0) for table in basis_t)
        values = []
        for layer in range(layers):
            both = jnp.concatenate(parts(rows_done[:, layer * RADIUS : (layer + 1) * RADIUS]), axis=1)
            values.append(
                jnp.dot(both, upper, preferred_element_type=F32) + jnp.dot(both, lower, preferred_element_type=F32)
            )
        total = summed(spectra, values, tile // 2, before)
    own[...], spill[...] = columns_half(total, basis, basis_t, 1, tile)
    send_half(xs, sends, own, spill)
    if early:
        place = halo("gx", xs[0]), edge("gy", 1)
        firsts[0][...] = stations[place].astype(F32) * (own[place[0], :] - observed[place])


def side_kernel(xs, early, other, tile, own, spill, observed, stations, *refs):
    count = len(xs)
    received, strips, refs = refs[:count], refs[count : 2 * count], refs[2 * count :]
    (predicted, residual, behind), sends = refs[:3], refs[3:]
    cols = edge("gy", other)
    predicted[...] = own[...]
    if count < 2:
        behind[...] = jnp.zeros_like(behind)
    for ref, strip, phase in zip(received, strips, xs):
        predicted[edge("gx", phase)] += ref[:RADIUS]
        rows = halo("gx", phase)
        behind[rows] = strip[1, :, cols] * (spill[rows] + ref[RADIUS:] - strip[0, :, cols])
    residual[...] = stations[:, cols].astype(F32) * (predicted[...] - observed[:, cols])
    for ref in sends:
        if early and other:
            ref[:RADIUS] = residual[edge("gx", xs[0])]
        else:
            ref[:tile] = residual[...]
        for k, phase in enumerate(xs):
            start = ref.shape[0] + (k - count) * RADIUS
            ref[start : start + RADIUS] = behind[halo("gx", phase)]


def scaled(spectra, layer, value, half):
    rows = []
    for a in range(4):
        blocks = [
            spectra[layer, group(a, half), group(b, half)]
            * value[a * half : (a + 1) * half, b * half : (b + 1) * half]
            for b in range(4)
        ]
        rows.append(jnp.concatenate(blocks, axis=1))
    return jnp.concatenate(rows, axis=0)


def gradient_half(spectra, value, basis, basis_t, other, tile, layers):
    low, high = slice(0, tile), slice(tile, 2 * tile)
    table = pair(basis, ALL, edge("gy", other))
    mixed = [wide_product(parts(scaled(spectra, layer, value, tile // 2)), table) for layer in range(layers)]
    mixed = jnp.concatenate(mixed, axis=1)
    return product(pair(basis_t, ALL, low), parts(mixed[low])) + product(
        pair(basis_t, ALL, high), parts(mixed[high])
    )


def own_kernel(tile, *refs):
    halves, basis = (refs[:3], refs[3:6]), refs[6:8]
    predicted_out, residual_out, rows_done, residual, behind, sems = refs[8:]
    low, high = slice(0, tile), slice(tile, 2 * tile)
    copies = []
    for k, other in enumerate((1, 0)):
        cols = edge("gy", other)
        copies.append(pltpu.make_async_copy(halves[k][0], predicted_out.at[:, cols], sems.at[2 * k]))
        copies.append(pltpu.make_async_copy(halves[k][1], residual_out.at[:, cols], sems.at[2 * k + 1]))
    for copy in copies:
        copy.start()
    for k, other in enumerate((1, 0)):
        residual[:, edge("gy", other)] = halves[k][1][...]
        behind[:, edge("gy", other)] = halves[k][2][...]
    rows_done[low] = product(pair(basis, low, ALL), parts(residual[...] + behind[...]))
    rows_done[high] = product(pair(basis, high, ALL), parts(residual[...] - behind[...]))
    for copy in copies:
        copy.wait()


def strip_rows(top, bottom, basis, tile):
    up = wide_product(pair(basis, slice(0, tile), ALL), parts(top + bottom))
    down = wide_product(pair(basis, slice(tile, 2 * tile), ALL), parts(top - bottom))
    return jnp.concatenate([up, down], axis=0)


def far_kernel(xs, paired, tile, layers, spectra, rows_done, *refs):
    strips, refs = refs[: len(paired)], refs[len(paired) :]
    basis, basis_t, (field, result, corner, wrapped) = refs[:2], refs[2:4], refs[4:]
    low, high = slice(0, tile), slice(tile, 2 * tile)
    wrapped[...] = jnp.zeros_like(wrapped)
    for ref, phase in zip(strips, paired):
        if len(xs) < 2:
            corner[...] = jnp.zeros_like(corner)
        for k, other in enumerate(xs):
            start = tile + k * RADIUS
            corner[halo("gx", other)] = ref[start : start + RADIUS]
        wrapped[:, halo("gy", phase)] = strip_rows(ref[:tile], corner[...], basis, tile)
    field[:, low] = product(parts(rows_done[...] + wrapped[...]), pair(basis_t, ALL, low))
    field[:, high] = product(parts(rows_done[...] - wrapped[...]), pair(basis_t, ALL, high))
    result[...] = gradient_half(spectra, field, basis, basis_t, 0, tile, layers)


def adjoint_kernel(xs, crossing, early, tile, layers, spectra, field, far, *refs):
    firsts, refs = refs[:early], refs[early:]
    strips, basis, basis_t = refs[: len(crossing)], refs[len(crossing) :][:2], refs[len(crossing) :][2:4]
    gradient, across, corner, held, result, sems = refs[len(crossing) + 4 :]
    low, high = slice(0, tile), slice(tile, 2 * tile)
    copies = []

    def put(source, first, other):
        for layer in range(layers):
            here = source.at[:, layer * RADIUS : (layer + 1) * RADIUS]
            there = gradient.at[layer, :, edge("gy", other)]
            copies.append(pltpu.make_async_copy(here, there, sems.at[first + layer]))
            copies[-1].start()

    put(far, 0, 0)
    for ref, phase in zip(strips, crossing):
        if len(xs) < 2:
            corner[...] = jnp.zeros_like(corner)
        if early:
            across[halo("gx", xs[0])] = firsts[0][...]
            across[edge("gx", xs[0])] = ref[:RADIUS]
        else:
            across[...] = ref[:tile]
        for k, other in enumerate(xs):
            start = ref.shape[0] + (k - len(xs)) * RADIUS
            corner[halo("gx", other)] = ref[start : start + RADIUS]
        both = jnp.concatenate(parts(strip_rows(across[...], corner[...], basis, tile)), axis=1)
        ticks = halo("gy", phase)
        upper, lower = (jnp.concatenate([table[ticks, :]] * 2, axis=0) for table in basis_t)
        value = jnp.dot(both, upper, preferred_element_type=F32) + jnp.dot(both, lower, preferred_element_type=F32)
        held[:, low] = field[:, low] + value[:, low]
        held[:, high] = field[:, high] - value[:, high]
    result[...] = gradient_half(spectra, held if crossing else field, basis, basis_t, 1, tile, layers)
    put(result, layers, 1)
    for copy in copies:
        copy.wait()


def partner(index, phase):
    return index + 1 if index % 2 == phase else index - 1


def swap(value, axis, phase):
    count = lax.axis_size(axis)
    links = [(i, partner(i, phase)) for i in range(count)]
    return lax.ppermute(value, axis, [link for link in links if 0 <= link[1] < count])


def in_hbm(value):
    return pltpu.with_memory_space_constraint(value, pltpu.HBM)


def phases(axis):
    return [phase for phase in (1, 0) if lax.axis_size(axis) > 1 + phase]


def cost(units, tile):
    flops = int(units * 6 * tile**3)
    return pl.CostEstimate(flops=flops, bytes_accessed=tile * tile * 16, transcendentals=0)


def body(density, observed, stations, layer_index):
    layers, tile = density.shape[0], density.shape[1]
    xs, ys = phases("gx"), phases("gy")
    groups = 3 * (tile // 2)
    consts = [jnp.asarray(table) for table in tables(tile)]
    basis, sides = consts[:4], consts[4:]
    vmem = pl.BlockSpec(memory_space=pltpu.VMEM)
    hbm = pl.BlockSpec(memory_space=pltpu.HBM)

    def array(*shape):
        return jax.ShapeDtypeStruct(shape, F32)

    def cols_of(phase):
        upper = (lax.axis_index("gy") & 1) == phase
        return jnp.where(upper, density[..., tile - RADIUS :], density[..., :RADIUS])

    def rows_of(phase):
        upper = (lax.axis_index("gx") & 1) == phase
        both = jnp.stack([observed, stations.astype(F32)])
        return jnp.where(upper, both[:, tile - RADIUS :], both[:, :RADIUS])

    density_halos = [swap(cols_of(phase), "gy", phase) for phase in ys]
    strips = [swap(rows_of(phase), "gx", phase) for phase in xs]
    paired = [phase for phase in ys if not phase]
    crossing = [phase for phase in ys if phase]
    early = int(len(xs) == 1 and 1 in ys)
    part = array(tile, RADIUS)
    operands = [in_hbm(value) for value in (layer_index, *sides)]
    operands += [density, *density_halos[len(crossing) :], *basis]
    spectra, before, *out = pl.pallas_call(
        functools.partial(prepare_kernel, xs, paired, tile, layers),
        out_shape=[array(layers, groups, groups), array(2 * tile, 2 * tile), part, part]
        + [array(2 * RADIUS, RADIUS)] * len(xs),
        in_specs=[hbm] * 5 + [vmem] * (len(operands) - 5),
        out_specs=[vmem] * (4 + len(xs)),
        scratch_shapes=[pltpu.VMEM(table.shape, BF16) for table in sides]
        + [
            pltpu.SMEM((layers,), jnp.int32),
            pltpu.VMEM((layers * tile, tile), F32),
            pltpu.VMEM((layers, 2 * tile, 2 * tile), F32),
            pltpu.SemaphoreType.DMA((5,)),
        ],
        compiler_params=PARAMS,
        cost_estimate=cost(24, tile),
        name="prepare",
    )(*operands)
    values, sends = {0: out[:2]}, {0: out[2:]}
    operands = [spectra, before, observed, stations, *density_halos[: len(crossing)], *basis]
    out = pl.pallas_call(
        functools.partial(forward_kernel, xs, crossing, early, tile, layers),
        out_shape=[part, part] + [array(2 * RADIUS, RADIUS)] * len(xs) + [array(tile - RADIUS, RADIUS)] * early,
        in_specs=[vmem] * len(operands),
        out_specs=[vmem] * (2 + len(xs) + early),
        compiler_params=PARAMS,
        cost_estimate=cost(12, tile),
        name="forward",
    )(*operands)
    values[1], sends[1], firsts = out[:2], out[2 : 2 + len(xs)], out[2 + len(xs) :]
    sums = {other: [swap(value, "gx", phase) for value, phase in zip(sends[other], xs)] for other in (1, 0)}
    firsts = [swap(value, "gy", 1) for value in firsts]
    halves, received = [], []
    for other in (1, 0):
        operands = [*values[other], observed, stations, *sums[other], *strips]
        there = int(other in ys)
        tall = RADIUS * len(xs) + (RADIUS if early and other else tile)
        out = pl.pallas_call(
            functools.partial(side_kernel, xs, early, other, tile),
            out_shape=[array(tile, RADIUS)] * 3 + [array(tall, RADIUS)] * there,
            in_specs=[vmem] * len(operands),
            out_specs=[vmem] * (3 + there),
            compiler_params=PARAMS,
            cost_estimate=cost(1, tile),
        )(*operands)
        halves += out[:3]
        received += [swap(value, "gy", other) for value in out[3:]]
    crossing = [phase for phase in ys if phase]
    paired = [phase for phase in ys if not phase]
    operands = [*halves, *basis[:2]]
    predicted, residual, rows_done = pl.pallas_call(
        functools.partial(own_kernel, tile),
        out_shape=[array(tile, tile)] * 2 + [array(2 * tile, tile)],
        in_specs=[vmem] * len(operands),
        out_specs=[hbm] * 2 + [vmem],
        scratch_shapes=[pltpu.VMEM((tile, tile), F32)] * 2 + [pltpu.SemaphoreType.DMA((4,))],
        compiler_params=PARAMS,
        cost_estimate=cost(2, tile),
        name="own",
    )(*operands)
    operands = [spectra, rows_done, *received[len(crossing) :], *basis]
    field, far = pl.pallas_call(
        functools.partial(far_kernel, xs, paired, tile, layers),
        out_shape=[array(2 * tile, 2 * tile), array(tile, layers * RADIUS)],
        in_specs=[vmem] * len(operands),
        out_specs=[vmem] * 2,
        scratch_shapes=[pltpu.VMEM((tile, RADIUS), F32), pltpu.VMEM((2 * tile, tile), F32)],
        compiler_params=PARAMS,
        cost_estimate=cost(14, tile),
        name="far",
    )(*operands)
    operands = [spectra, field, far, *firsts, *received[: len(crossing)], *basis]
    gradient = pl.pallas_call(
        functools.partial(adjoint_kernel, xs, crossing, early, tile, layers),
        out_shape=array(layers, tile, tile),
        in_specs=[vmem] * len(operands),
        out_specs=hbm,
        scratch_shapes=[pltpu.VMEM((tile, RADIUS), F32)] * 2
        + [
            pltpu.VMEM((2 * tile, 2 * tile), F32),
            pltpu.VMEM((tile, layers * RADIUS), F32),
            pltpu.SemaphoreType.DMA((2 * layers,)),
        ],
        compiler_params=PARAMS,
        cost_estimate=cost(12, tile),
        name="adjoint",
    )(*operands)
    return predicted, residual, gradient


def solution(mesh):
    in_specs = (P(None, "gx", "gy"), P("gx", "gy"), P("gx", "gy"), P())
    out_specs = (P("gx", "gy"), P("gx", "gy"), P(None, "gx", "gy"))
    return jax.shard_map(body, mesh=mesh, in_specs=in_specs, out_specs=out_specs, check_vma=False)
```

```python
import functools
import math

import jax
import jax.numpy as jnp
import ml_dtypes
import numpy as np
from jax import lax
from jax.experimental import pallas as pl
from jax.experimental.pallas import tpu as pltpu
from jax.sharding import PartitionSpec as P


RADIUS = 128
LAYERS_ALL = 512

F32 = jnp.float32
BF16 = jnp.bfloat16
PARAMS = pltpu.CompilerParams(vmem_limit_bytes=24 * 2**20)


def halves(table):
    table = table.astype(np.float32)
    high = table.astype(ml_dtypes.bfloat16)
    low = (table - high.astype(np.float32)).astype(ml_dtypes.bfloat16)
    return [high, low]


@functools.lru_cache(maxsize=None)
def tables(tile):
    length = 2 * tile
    half = tile // 2
    ticks = np.arange(tile)
    even = 2 * np.arange(half)
    odd = even + 1

    def angles(freqs):
        return (freqs[:, None] * ticks[None, :] % length) * (2.0 * math.pi / length)

    middle = even.copy()
    middle[0] = tile
    even_sin = np.sin(angles(even))
    even_sin[0] = np.cos(angles(middle))[0]
    basis = np.concatenate([np.cos(angles(even)), even_sin, np.cos(angles(odd)), np.sin(angles(odd))])
    fold = np.where(ticks == 0, 1.0, 2.0) * (ticks <= RADIUS)
    freqs = np.concatenate([even, middle, odd])
    weights = np.where((freqs == 0) | (freqs == tile), 1.0, 2.0) / length
    sides = np.cos(angles(freqs)) * fold[None, :] * weights[:, None]
    return halves(basis) + halves(basis.T) + halves(sides) + halves(sides.T)


def parts(value):
    high = value.astype(BF16)
    return high, (value - high.astype(F32)).astype(BF16)


def product(left, right):
    def dot(a, b):
        return jnp.dot(a, b, preferred_element_type=F32)

    return dot(left[0], right[0]) + (dot(left[0], right[1]) + dot(left[1], right[0]))


def wide_product(left, right):
    width = right[0].shape[1]
    both = jnp.dot(left[0], jnp.concatenate(right, axis=1), preferred_element_type=F32)
    return both[:, :width] + (both[:, width:] + jnp.dot(left[1], right[0], preferred_element_type=F32))


def pair(refs, *index):
    return refs[0][index], refs[1][index]


def side(axis, phase):
    return jnp.where((lax.axis_index(axis) & 1) == phase, 0, RADIUS)


def halo(axis, phase):
    return pl.ds(pl.multiple_of(side(axis, phase), RADIUS), RADIUS)


def edge(axis, phase):
    return pl.ds(pl.multiple_of(RADIUS - side(axis, phase), RADIUS), RADIUS)


def group(block, half):
    return slice(min(block, 2) * half, (min(block, 2) + 1) * half)


ALL = slice(None)


def columns_half(total, basis, basis_t, other, tile):
    low, high = slice(0, tile), slice(tile, 2 * tile)
    mixed = wide_product(parts(total), pair(basis, ALL, edge("gy", other)))
    even = wide_product(pair(basis_t, ALL, low), parts(mixed[low]))
    odd = wide_product(pair(basis_t, ALL, high), parts(mixed[high]))
    return even + odd, even - odd


def send_half(xs, sends, own, spill):
    for ref, phase in zip(sends, xs):
        ref[:RADIUS] = spill[halo("gx", phase)]
        ref[RADIUS:] = own[edge("gx", phase)]


def summed(spectra, values, half, before=None):
    rows = []
    for a in range(4):
        blocks = []
        for b in range(4):
            place = slice(a * half, (a + 1) * half), slice(b * half, (b + 1) * half)
            block = None
            for layer, value in enumerate(values):
                term = spectra[layer, group(a, half), group(b, half)] * value[place]
                block = term if block is None else block + term
            if before is not None:
                block = before[place] + block if b < 2 else before[place] - block
            blocks.append(block)
        rows.append(jnp.concatenate(blocks, axis=1))
    return jnp.concatenate(rows, axis=0)


def prepare_kernel(xs, paired, tile, layers, index_source, *refs):
    sources, density, refs = refs[:4], refs[4], refs[5:]
    received, refs = refs[: len(paired)], refs[len(paired) :]
    basis, basis_t, (spectra, total, own, spill), refs = refs[:2], refs[2:4], refs[4:8], refs[8:]
    sends, held, (index, wrapped, fields, sems) = refs[: len(xs)], refs[len(xs) : len(xs) + 4], refs[len(xs) + 4 :]
    copies = [pltpu.make_async_copy(sources[k], held[k], sems.at[k]) for k in range(4)]
    copies.append(pltpu.make_async_copy(index_source, index, sems.at[4]))
    for copy in reversed(copies):
        copy.start()
    low, high = slice(0, tile), slice(tile, 2 * tile)
    wrapped[...] = jnp.zeros_like(wrapped)
    for ref, phase in zip(received, paired):
        for layer in range(layers):
            wrapped[layer * tile : (layer + 1) * tile, halo("gy", phase)] = ref[layer]
    field = jnp.concatenate([density[layer] for layer in range(layers)], axis=0)
    behind = wrapped[...]
    even = product(parts(field + behind), pair(basis_t, ALL, low))
    odd = product(parts(field - behind), pair(basis_t, ALL, high))
    for layer in range(layers):
        rows = slice(layer * tile, (layer + 1) * tile)
        both = jnp.concatenate([even[rows], odd[rows]], axis=1)
        fields[layer] = product(pair(basis, ALL, ALL), parts(both))
    span = RADIUS + 8
    rows = lax.broadcasted_iota(jnp.int32, (span, tile), 0)
    cols = lax.broadcasted_iota(jnp.int32, (span, tile), 1)
    offsets = (rows * rows + cols * cols).astype(F32)
    copies[4].wait()
    values = []
    for layer in range(layers):
        depth = RADIUS * (0.375 + index[layer].astype(F32) / LAYERS_ALL)
        square = offsets + depth * depth
        values.append(depth * depth / (square * jnp.sqrt(square)))
    copies[2].wait()
    copies[3].wait()
    first = product(parts(jnp.concatenate(values, axis=0)), pair(held[2:], ALL, ALL))
    copies[0].wait()
    copies[1].wait()
    rest = jnp.zeros((tile - span, first.shape[1]), F32)
    for layer in range(layers):
        whole = jnp.concatenate([first[layer * span : (layer + 1) * span], rest], axis=0)
        spectra[layer] = product(pair(held[:2], ALL, ALL), parts(whole))
    total[...] = summed(spectra, [fields.at[layer] for layer in range(layers)], tile // 2)
    own[...], spill[...] = columns_half(total[...], basis, basis_t, 0, tile)
    send_half(xs, sends, own, spill)


def forward_kernel(xs, crossing, early, tile, layers, spectra, before, observed, stations, *refs):
    received, refs = refs[: len(crossing)], refs[len(crossing) :]
    basis, basis_t, (own, spill), refs = refs[:2], refs[2:4], refs[4:6], refs[6:]
    sends, firsts = refs[: len(xs)], refs[len(xs) :]
    total = before[...]
    for ref, phase in zip(received, crossing):
        strips = jnp.concatenate([ref[layer] for layer in range(layers)], axis=1)
        rows_done = product(pair(basis, ALL, ALL), parts(strips))
        ticks = halo("gy", phase)
        upper, lower = (jnp.concatenate([table[ticks, :]] * 2, axis=0) for table in basis_t)
        values = []
        for layer in range(layers):
            both = jnp.concatenate(parts(rows_done[:, layer * RADIUS : (layer + 1) * RADIUS]), axis=1)
            values.append(
                jnp.dot(both, upper, preferred_element_type=F32) + jnp.dot(both, lower, preferred_element_type=F32)
            )
        total = summed(spectra, values, tile // 2, before)
    own[...], spill[...] = columns_half(total, basis, basis_t, 1, tile)
    send_half(xs, sends, own, spill)
    if early:
        place = halo("gx", xs[0]), edge("gy", 1)
        firsts[0][...] = stations[place].astype(F32) * (own[place[0], :] - observed[place])


def side_kernel(xs, early, other, tile, own, spill, observed, stations, *refs):
    count = len(xs)
    received, strips, refs = refs[:count], refs[count : 2 * count], refs[2 * count :]
    (predicted, residual, behind), sends = refs[:3], refs[3:]
    cols = edge("gy", other)
    predicted[...] = own[...]
    if count < 2:
        behind[...] = jnp.zeros_like(behind)
    for ref, strip, phase in zip(received, strips, xs):
        predicted[edge("gx", phase)] += ref[:RADIUS]
        rows = halo("gx", phase)
        behind[rows] = strip[1, :, cols] * (spill[rows] + ref[RADIUS:] - strip[0, :, cols])
    residual[...] = stations[:, cols].astype(F32) * (predicted[...] - observed[:, cols])
    for ref in sends:
        if early and other:
            ref[:RADIUS] = residual[edge("gx", xs[0])]
        else:
            ref[:tile] = residual[...]
        for k, phase in enumerate(xs):
            start = ref.shape[0] + (k - count) * RADIUS
            ref[start : start + RADIUS] = behind[halo("gx", phase)]


def scaled(spectra, layer, value, half):
    rows = []
    for a in range(4):
        blocks = [
            spectra[layer, group(a, half), group(b, half)]
            * value[a * half : (a + 1) * half, b * half : (b + 1) * half]
            for b in range(4)
        ]
        rows.append(jnp.concatenate(blocks, axis=1))
    return jnp.concatenate(rows, axis=0)


def gradient_half(spectra, value, basis, basis_t, other, tile, layers, pieces=(ALL,)):
    low, high = slice(0, tile), slice(tile, 2 * tile)
    table = pair(basis, ALL, edge("gy", other))
    mixed = [wide_product(parts(scaled(spectra, layer, value, tile // 2)), table) for layer in range(layers)]
    mixed = jnp.concatenate(mixed, axis=1)
    even, odd = parts(mixed[low]), parts(mixed[high])
    for rows in pieces:
        yield rows, product(pair(basis_t, rows, low), even) + product(pair(basis_t, rows, high), odd)


def own_kernel(tile, *refs):
    halves, basis = (refs[:3], refs[3:6]), refs[6:8]
    predicted_out, residual_out, rows_done, residual, behind, sems = refs[8:]
    low, high = slice(0, tile), slice(tile, 2 * tile)
    copies = []
    for k, other in enumerate((1, 0)):
        cols = edge("gy", other)
        copies.append(pltpu.make_async_copy(halves[k][0], predicted_out.at[:, cols], sems.at[2 * k]))
        copies.append(pltpu.make_async_copy(halves[k][1], residual_out.at[:, cols], sems.at[2 * k + 1]))
    for copy in copies:
        copy.start()
    for k, other in enumerate((1, 0)):
        residual[:, edge("gy", other)] = halves[k][1][...]
        behind[:, edge("gy", other)] = halves[k][2][...]
    rows_done[low] = product(pair(basis, low, ALL), parts(residual[...] + behind[...]))
    rows_done[high] = product(pair(basis, high, ALL), parts(residual[...] - behind[...]))
    for copy in copies:
        copy.wait()


def strip_rows(top, bottom, basis, tile):
    up = wide_product(pair(basis, slice(0, tile), ALL), parts(top + bottom))
    down = wide_product(pair(basis, slice(tile, 2 * tile), ALL), parts(top - bottom))
    return jnp.concatenate([up, down], axis=0)


def far_kernel(xs, paired, tile, layers, spectra, rows_done, *refs):
    strips, refs = refs[: len(paired)], refs[len(paired) :]
    basis, basis_t, (field, result, corner, wrapped) = refs[:2], refs[2:4], refs[4:]
    low, high = slice(0, tile), slice(tile, 2 * tile)
    wrapped[...] = jnp.zeros_like(wrapped)
    for ref, phase in zip(strips, paired):
        if len(xs) < 2:
            corner[...] = jnp.zeros_like(corner)
        for k, other in enumerate(xs):
            start = tile + k * RADIUS
            corner[halo("gx", other)] = ref[start : start + RADIUS]
        wrapped[:, halo("gy", phase)] = strip_rows(ref[:tile], corner[...], basis, tile)
    field[:, low] = product(parts(rows_done[...] + wrapped[...]), pair(basis_t, ALL, low))
    field[:, high] = product(parts(rows_done[...] - wrapped[...]), pair(basis_t, ALL, high))
    for rows, value in gradient_half(spectra, field, basis, basis_t, 0, tile, layers):
        result[rows] = value


def adjoint_kernel(xs, crossing, early, tile, layers, spectra, field, far, *refs):
    firsts, refs = refs[:early], refs[early:]
    strips, basis, basis_t = refs[: len(crossing)], refs[len(crossing) :][:2], refs[len(crossing) :][2:4]
    gradient, across, corner, held, result, sems = refs[len(crossing) + 4 :]
    low, high = slice(0, tile), slice(tile, 2 * tile)
    copies = []

    def put(source, rows, other):
        for layer in range(layers):
            here = source.at[rows, layer * RADIUS : (layer + 1) * RADIUS]
            there = gradient.at[layer, rows, edge("gy", other)]
            copies.append(pltpu.make_async_copy(here, there, sems.at[len(copies)]))
            copies[-1].start()

    put(far, slice(0, tile), 0)
    for ref, phase in zip(strips, crossing):
        if len(xs) < 2:
            corner[...] = jnp.zeros_like(corner)
        if early:
            across[halo("gx", xs[0])] = firsts[0][...]
            across[edge("gx", xs[0])] = ref[:RADIUS]
        else:
            across[...] = ref[:tile]
        for k, other in enumerate(xs):
            start = ref.shape[0] + (k - len(xs)) * RADIUS
            corner[halo("gx", other)] = ref[start : start + RADIUS]
        both = jnp.concatenate(parts(strip_rows(across[...], corner[...], basis, tile)), axis=1)
        ticks = halo("gy", phase)
        upper, lower = (jnp.concatenate([table[ticks, :]] * 2, axis=0) for table in basis_t)
        value = jnp.dot(both, upper, preferred_element_type=F32) + jnp.dot(both, lower, preferred_element_type=F32)
        held[:, low] = field[:, low] + value[:, low]
        held[:, high] = field[:, high] - value[:, high]
    total = held if crossing else field
    pieces = [slice(start, start + tile // 2) for start in range(0, tile, tile // 2)]
    for rows, value in gradient_half(spectra, total, basis, basis_t, 1, tile, layers, pieces):
        result[rows] = value
        put(result, rows, 1)
    for copy in copies:
        copy.wait()


def partner(index, phase):
    return index + 1 if index % 2 == phase else index - 1


def swap(value, axis, phase):
    count = lax.axis_size(axis)
    links = [(i, partner(i, phase)) for i in range(count)]
    return lax.ppermute(value, axis, [link for link in links if 0 <= link[1] < count])


def in_hbm(value):
    return pltpu.with_memory_space_constraint(value, pltpu.HBM)


def phases(axis):
    return [phase for phase in (1, 0) if lax.axis_size(axis) > 1 + phase]


def cost(units, tile):
    flops = int(units * 6 * tile**3)
    return pl.CostEstimate(flops=flops, bytes_accessed=tile * tile * 16, transcendentals=0)


def body(density, observed, stations, layer_index):
    layers, tile = density.shape[0], density.shape[1]
    xs, ys = phases("gx"), phases("gy")
    groups = 3 * (tile // 2)
    consts = [jnp.asarray(table) for table in tables(tile)]
    basis, sides = consts[:4], consts[4:]
    vmem = pl.BlockSpec(memory_space=pltpu.VMEM)
    hbm = pl.BlockSpec(memory_space=pltpu.HBM)

    def array(*shape):
        return jax.ShapeDtypeStruct(shape, F32)

    def cols_of(phase):
        upper = (lax.axis_index("gy") & 1) == phase
        return jnp.where(upper, density[..., tile - RADIUS :], density[..., :RADIUS])

    def rows_of(phase):
        upper = (lax.axis_index("gx") & 1) == phase
        both = jnp.stack([observed, stations.astype(F32)])
        return jnp.where(upper, both[:, tile - RADIUS :], both[:, :RADIUS])

    density_halos = [swap(cols_of(phase), "gy", phase) for phase in ys]
    strips = [swap(rows_of(phase), "gx", phase) for phase in xs]
    paired = [phase for phase in ys if not phase]
    crossing = [phase for phase in ys if phase]
    early = int(len(xs) == 1 and 1 in ys)
    part = array(tile, RADIUS)
    operands = [in_hbm(value) for value in (layer_index, *sides)]
    operands += [density, *density_halos[len(crossing) :], *basis]
    spectra, before, *out = pl.pallas_call(
        functools.partial(prepare_kernel, xs, paired, tile, layers),
        out_shape=[array(layers, groups, groups), array(2 * tile, 2 * tile), part, part]
        + [array(2 * RADIUS, RADIUS)] * len(xs),
        in_specs=[hbm] * 5 + [vmem] * (len(operands) - 5),
        out_specs=[vmem] * (4 + len(xs)),
        scratch_shapes=[pltpu.VMEM(table.shape, BF16) for table in sides]
        + [
            pltpu.SMEM((layers,), jnp.int32),
            pltpu.VMEM((layers * tile, tile), F32),
            pltpu.VMEM((layers, 2 * tile, 2 * tile), F32),
            pltpu.SemaphoreType.DMA((5,)),
        ],
        compiler_params=PARAMS,
        cost_estimate=cost(24, tile),
        name="prepare",
    )(*operands)
    values, sends = {0: out[:2]}, {0: out[2:]}
    operands = [spectra, before, observed, stations, *density_halos[: len(crossing)], *basis]
    out = pl.pallas_call(
        functools.partial(forward_kernel, xs, crossing, early, tile, layers),
        out_shape=[part, part] + [array(2 * RADIUS, RADIUS)] * len(xs) + [array(tile - RADIUS, RADIUS)] * early,
        in_specs=[vmem] * len(operands),
        out_specs=[vmem] * (2 + len(xs) + early),
        compiler_params=PARAMS,
        cost_estimate=cost(12, tile),
        name="forward",
    )(*operands)
    values[1], sends[1], firsts = out[:2], out[2 : 2 + len(xs)], out[2 + len(xs) :]
    sums = {other: [swap(value, "gx", phase) for value, phase in zip(sends[other], xs)] for other in (1, 0)}
    firsts = [swap(value, "gy", 1) for value in firsts]
    halves, received = [], []
    for other in (1, 0):
        operands = [*values[other], observed, stations, *sums[other], *strips]
        there = int(other in ys)
        tall = RADIUS * len(xs) + (RADIUS if early and other else tile)
        out = pl.pallas_call(
            functools.partial(side_kernel, xs, early, other, tile),
            out_shape=[array(tile, RADIUS)] * 3 + [array(tall, RADIUS)] * there,
            in_specs=[vmem] * len(operands),
            out_specs=[vmem] * (3 + there),
            compiler_params=PARAMS,
            cost_estimate=cost(1, tile),
        )(*operands)
        halves += out[:3]
        received += [swap(value, "gy", other) for value in out[3:]]
    crossing = [phase for phase in ys if phase]
    paired = [phase for phase in ys if not phase]
    operands = [*halves, *basis[:2]]
    predicted, residual, rows_done = pl.pallas_call(
        functools.partial(own_kernel, tile),
        out_shape=[array(tile, tile)] * 2 + [array(2 * tile, tile)],
        in_specs=[vmem] * len(operands),
        out_specs=[hbm] * 2 + [vmem],
        scratch_shapes=[pltpu.VMEM((tile, tile), F32)] * 2 + [pltpu.SemaphoreType.DMA((4,))],
        compiler_params=PARAMS,
        cost_estimate=cost(2, tile),
        name="own",
    )(*operands)
    operands = [spectra, rows_done, *received[len(crossing) :], *basis]
    field, far = pl.pallas_call(
        functools.partial(far_kernel, xs, paired, tile, layers),
        out_shape=[array(2 * tile, 2 * tile), array(tile, layers * RADIUS)],
        in_specs=[vmem] * len(operands),
        out_specs=[vmem] * 2,
        scratch_shapes=[pltpu.VMEM((tile, RADIUS), F32), pltpu.VMEM((2 * tile, tile), F32)],
        compiler_params=PARAMS,
        cost_estimate=cost(14, tile),
        name="far",
    )(*operands)
    operands = [spectra, field, far, *firsts, *received[: len(crossing)], *basis]
    gradient = pl.pallas_call(
        functools.partial(adjoint_kernel, xs, crossing, early, tile, layers),
        out_shape=array(layers, tile, tile),
        in_specs=[vmem] * len(operands),
        out_specs=hbm,
        scratch_shapes=[pltpu.VMEM((tile, RADIUS), F32)] * 2
        + [
            pltpu.VMEM((2 * tile, 2 * tile), F32),
            pltpu.VMEM((tile, layers * RADIUS), F32),
            pltpu.SemaphoreType.DMA((3 * layers,)),
        ],
        compiler_params=PARAMS,
        cost_estimate=cost(12, tile),
        name="adjoint",
    )(*operands)
    return predicted, residual, gradient


def solution(mesh):
    in_specs = (P(None, "gx", "gy"), P("gx", "gy"), P("gx", "gy"), P())
    out_specs = (P("gx", "gy"), P("gx", "gy"), P(None, "gx", "gy"))
    return jax.shard_map(body, mesh=mesh, in_specs=in_specs, out_specs=out_specs, check_vma=False)
```
